32 devices in a mesh: row: 4 (over y, x), col: 8 (over z, core).
Axes of the slice: x: 2, y: 2, z: 4, core: 2. Of those that a mesh axis runs over, the one named last changes fastest.
Arguments:
- user_feats: bfloat16 [4096, 128], P(('row', 'col')), may hold values from -6 to 6
- item_feats: bfloat16 [16384, 128], P(('col', 'row')), may hold values from -6 to 6
- tile_values: bfloat16 [4, 8, 1, 512, 512], P('row', 'col'), may hold values from -0.15625 to 0.15625
- tile_coords: int32 [4, 8, 2, 1], P('row', 'col'), may hold values from 0 to 3, as said below
- tile_count: int32 [4, 8], P('row', 'col'), may hold values from 1 to 1, as said below
Outputs:
- users_next: bfloat16 [4096, 128], P(('row', 'col'))
- items_next: bfloat16 [16384, 128], P(('col', 'row'))
The draws below stay inside these ranges and needn't reach their ends.
Inputs may be any that keep to these rules, and one draw needn't show every extreme that they name: `tile_coords`: within one device's first tile_count slots the pairs (user tile, item tile) are distinct; the first entry is a user tile below 2, the second an item tile below 4; slots at or after the count carry no tile. `tile_count`: at least one device has all 1 slots live.
All inputs are finite; a program needn't handle non-finite values.
Results may differ from the reference program's by a relative error of at most 0.001.
Values may be sent and summed in bfloat16 or wider, within the bound.
A program may use at most 64 MiB of HBM per device.

```python
import jax
import jax.numpy as jnp
from jax import lax

W = 128
TS = 512
UT = 2
IT = 4
MAXT = 1
USERS = 4096
ITEMS = 16384
N_ROW = 4
N_COL = 8


def draw_tile_coords(key, part):
    keys = jax.random.split(jax.random.fold_in(key, 7), N_ROW * N_COL)
    perms = jax.vmap(lambda single: jax.random.permutation(single, UT * IT))(keys)
    places = perms[:, :MAXT].reshape(N_ROW, N_COL, MAXT).astype(jnp.int32)
    return jnp.stack([places // IT, places % IT], axis=2).astype(jnp.int32)


def draw_tile_count(key, part):
    first, second, third = jax.random.split(jax.random.fold_in(key, 11), 3)
    draw_one = jax.random.randint(first, (N_ROW * N_COL,), 1, MAXT + 1)
    draw_two = jax.random.randint(second, (N_ROW * N_COL,), 1, MAXT + 1)
    counts = jnp.minimum(draw_one, draw_two)
    busiest = jax.random.randint(third, (), 0, N_ROW * N_COL)
    counts = jnp.where(jnp.arange(N_ROW * N_COL) == busiest, MAXT, counts)
    return counts.reshape(N_ROW, N_COL).astype(jnp.int32)


def steps_of(stream_key, dims, cuts, least, largest):
    def one(dim, shards_of):
        steps = jax.random.uniform(jax.random.fold_in(jax.random.fold_in(stream_key, 6), dim), (shards_of,), jnp.float32, least / len(cuts), largest / len(cuts))
        return jnp.repeat(jnp.exp(steps), dims[dim] // shards_of).reshape((-1,) + (1,) * (len(dims) - dim - 1))

    factor_of = one(*cuts[0])
    for cut in cuts[1:]:
        factor_of = factor_of * one(*cut)
    return factor_of


def centred(rng, shape, deviation, bound, shards=(), dtype=jnp.bfloat16):
    loudness = steps_of(rng, shape, shards, -0.22, 0.18) if shards else 1.0
    values = jax.random.normal(rng, shape, jnp.float32) * deviation * loudness
    return jnp.minimum(jnp.maximum(values, -bound), bound).astype(dtype)


def setup_inputs(seed: int = 0) -> dict:
    key_of = jax.random.split(jax.random.key(seed), 6)
    user_feats = centred(key_of[0], (USERS, W), 1.0, 6.0, ((0, 32),))
    item_feats = centred(key_of[1], (ITEMS, W), 1.0, 6.0, ((0, 32),))
    tile_values = centred(key_of[2], (N_ROW, N_COL, MAXT, TS, TS), (3 * TS) ** -0.5, 0.15625, ((0, 4), (1, 8)))
    tile_coords = draw_tile_coords(jax.random.fold_in(key_of[5], 71), 0)
    tile_count = draw_tile_count(jax.random.fold_in(key_of[5], 71), 0)
    return dict(user_feats=user_feats, item_feats=item_feats, tile_values=tile_values, tile_coords=tile_coords, tile_count=tile_count)


def reference(user_feats, item_feats, tile_values, tile_coords, tile_count):
    total = N_ROW * N_COL * MAXT

    def step(index, carry):
        acc_users, acc_items = carry
        index = jnp.asarray(index).astype(jnp.int32)
        device = index // MAXT
        slot = index % MAXT
        row_id = device // N_COL
        col_id = device % N_COL
        tile = tile_values[row_id, col_id, slot]
        user_tile = tile_coords[row_id, col_id, 0, slot].astype(jnp.int32)
        item_tile = tile_coords[row_id, col_id, 1, slot].astype(jnp.int32)
        live = slot < tile_count[row_id, col_id]
        user_start = ((row_id * UT + user_tile) * TS).astype(jnp.int32)
        item_start = ((col_id * IT + item_tile) * TS).astype(jnp.int32)
        item_part = lax.dynamic_slice_in_dim(item_feats, item_start, TS, 0)
        user_part = lax.dynamic_slice_in_dim(user_feats, user_start, TS, 0)
        to_users = jnp.dot(tile, item_part, preferred_element_type=jnp.float32)
        to_items = jnp.dot(tile.T, user_part, preferred_element_type=jnp.float32)
        to_users = jnp.where(live, to_users, jnp.zeros_like(to_users))
        to_items = jnp.where(live, to_items, jnp.zeros_like(to_items))
        old_users = lax.dynamic_slice_in_dim(acc_users, user_start, TS, 0)
        old_items = lax.dynamic_slice_in_dim(acc_items, item_start, TS, 0)
        acc_users = lax.dynamic_update_slice_in_dim(acc_users, old_users + to_users, user_start, 0)
        acc_items = lax.dynamic_update_slice_in_dim(acc_items, old_items + to_items, item_start, 0)
        return acc_users, acc_items

    start = (jnp.zeros((USERS, W), jnp.float32), jnp.zeros((ITEMS, W), jnp.float32))
    acc_users, acc_items = lax.fori_loop(jnp.int32(0), jnp.int32(total), step, start)
    return acc_users.astype(jnp.bfloat16), acc_items.astype(jnp.bfloat16)
```

```python
import functools

import jax
import jax.numpy as jnp
from jax import lax
from jax.experimental import pallas as pl
from jax.experimental.pallas import tpu as pltpu
from jax.sharding import PartitionSpec as P

MESH = pl.DeviceIdType.MESH
STEPS = 32760.0
TINY = 1e-30


def gathered(user_feats, item_feats, tile_values, tile_coords, tile_count):
    user_block = lax.all_gather(user_feats, "col", axis=0, tiled=True)
    item_block = lax.all_gather(item_feats, "row", axis=0, tiled=True)
    tiles = tile_values[0, 0]
    coords = tile_coords[0, 0]
    count = tile_count[0, 0]
    slots = tiles.shape[0]
    size = tiles.shape[1]
    width = user_block.shape[1]
    user_tiles = user_block.shape[0] // size
    item_tiles = item_block.shape[0] // size
    live = jnp.arange(slots) < count
    pick_user = ((coords[0][:, None] == jnp.arange(user_tiles)[None, :]) & live[:, None]).astype(
        jnp.bfloat16
    )
    pick_item = (coords[1][:, None] == jnp.arange(item_tiles)[None, :]).astype(jnp.bfloat16)
    user_sel = jnp.einsum(
        "su,uiw->siw",
        pick_user,
        user_block.reshape(user_tiles, size, width),
        preferred_element_type=jnp.float32,
    ).astype(jnp.bfloat16)
    item_sel = jnp.einsum(
        "st,tjw->sjw",
        pick_item,
        item_block.reshape(item_tiles, size, width),
        preferred_element_type=jnp.float32,
    ).astype(jnp.bfloat16)
    to_users = jnp.einsum("sij,sjw->siw", tiles, item_sel, preferred_element_type=jnp.float32)
    to_items = jnp.einsum("sij,siw->sjw", tiles, user_sel, preferred_element_type=jnp.float32)
    part_users = jnp.einsum(
        "su,siw->uiw", pick_user.astype(jnp.float32), to_users, precision=lax.Precision.HIGHEST
    ).reshape(user_tiles * size, width)
    part_items = jnp.einsum(
        "st,sjw->tjw", pick_item.astype(jnp.float32), to_items, precision=lax.Precision.HIGHEST
    ).reshape(item_tiles * size, width)
    users_next = lax.psum_scatter(part_users, "col", scatter_dimension=0, tiled=True)
    items_next = lax.psum_scatter(part_items, "row", scatter_dimension=0, tiled=True)
    return (users_next.astype(jnp.bfloat16), items_next.astype(jnp.bfloat16))


def encode(values):
    rows, width = values.shape
    groups = values.reshape(rows // 8, 8, width)
    peak = jnp.maximum(jnp.max(jnp.abs(groups), axis=0), TINY)
    return encode_by(values, peak), peak


def encode_by(values, peak):
    rows, width = values.shape
    groups = values.reshape(rows // 8, 8, width)
    scaled = jnp.round(groups * (STEPS / peak)[None])
    return scaled.astype(jnp.int32).astype(jnp.int16).reshape(rows, width)


def decode(code, peak):
    rows, width = code.shape
    groups = code.astype(jnp.int32).astype(jnp.float32).reshape(rows // 8, 8, width)
    return (groups * (peak * (1.0 / STEPS))[None]).reshape(rows, width)


def kernel(
    n_z,
    coords_in,
    count_in,
    user_in,
    item_in,
    tile_in,
    out_u,
    out_i,
    u_all,
    i_all,
    tile_v,
    tile_t,
    meta,
    metas,
    part_u,
    from_p,
    send_z,
    peak_z,
    from_z,
    from_zp,
    part_i,
    send_1,
    peak_1,
    from_1,
    from_1p,
    send_2,
    peak_2,
    from_2,
    from_2p,
    coords,
    count,
    load_sem,
    meta_s,
    meta_r,
    uz_s,
    uz_r,
    up_s,
    up_r,
    ig_s,
    ig_r,
    rp_s,
    rp_r,
    rz_s,
    rz_r,
    rzp_s,
    rzp_r,
    r1_s,
    r1_r,
    r1p_s,
    r1p_r,
    r2_s,
    r2_r,
    r2p_s,
    r2p_r,
):
    row, col = lax.axis_index("row"), lax.axis_index("col")
    y, x = row // 2, row % 2
    z, core = col // 2, col % 2
    row_x, row_y = 2 * y + 1 - x, 2 * (1 - y) + x
    x_dev, y_dev = (row_x, col), (row_y, col)
    p_dev = (row, 2 * z + 1 - core)

    def far_first(at):
        flip = z // (n_z // 2)
        mirrored = z + flip * (n_z - 1 - 2 * z)
        to = n_z - 1 - at
        to = jnp.where(to <= mirrored, to - 1, to)
        return to + flip * (n_z - 1 - 2 * to)

    others = [far_first(at) for at in range(n_z - 1)]
    z_devs = [(row, 2 * at + core) for at in others]
    near_first = others[::-1]
    rows_u, rows_i = user_in.shape[0], item_in.shape[0]
    size = tile_v.shape[-1]
    chunk = rows_i // 4
    pieces = size // rows_u // 2

    def user_slot(at):
        blocks = size // rows_u
        inner = pl.multiple_of(at % blocks * rows_u, rows_u)
        return u_all.at[at // blocks, pl.ds(inner, rows_u)]

    def item_slot(at, part, parts=2):
        rows = rows_i // parts
        return i_all.at[at, pl.ds(part * rows, rows)]

    def copy(src, dst, send, recv, device):
        return pltpu.make_async_remote_copy(
            src_ref=src,
            dst_ref=dst,
            send_sem=send,
            recv_sem=recv,
            device_id=device,
            device_id_type=MESH,
        )

    def arrived(like, recv):
        copy(like, like, recv, recv, x_dev).wait_recv()

    def left(like, send):
        copy(like, like, send, send, x_dev).wait_send()

    barrier = pltpu.get_barrier_semaphore()
    peers = [x_dev, y_dev, p_dev] + z_devs
    for peer in peers:
        pl.semaphore_signal(barrier, inc=1, device_id=peer, device_id_type=MESH)
    loads = [
        pltpu.make_async_copy(user_in, user_slot(col), load_sem.at[0]),
        pltpu.make_async_copy(item_in, i_all.at[row], load_sem.at[1]),
        pltpu.make_async_copy(tile_in, tile_v, load_sem.at[2]),
        pltpu.make_async_copy(coords_in, coords, load_sem.at[3]),
        pltpu.make_async_copy(count_in, count, load_sem.at[4]),
    ]
    for load in loads:
        load.start()

    loads[3].wait()
    loads[4].wait()
    tu, ti = coords[0], coords[1]
    meta[0] = jnp.full(meta.shape[1:], tu, jnp.int32)
    meta[1] = jnp.full(meta.shape[1:], ti, jnp.int32)
    meta[2] = jnp.full(meta.shape[1:], count[0, 0], jnp.int32)
    my_tu, my_ti, live = meta[0][0:1, :], meta[1][0:1, :], meta[2][0:1, :] > 0
    pl.semaphore_wait(barrier, len(peers))

    def relay_item(at, part, recv, device):
        piece = item_slot(at, part, 4)
        copy(piece, piece, ig_s.at[0], ig_r.at[recv], device).start()

    loads[0].wait()
    own = user_slot(col)
    for device in z_devs:
        copy(own, own, uz_s.at[0], uz_r.at[z], device).start()
    copy(own, own, up_s.at[0], up_r.at[0], p_dev).start()
    loads[1].wait()
    for part in range(2):
        relay_item(row, part, part, x_dev)
        relay_item(row, 2 + part, 2 + part, y_dev)
    for part, device in ((1, x_dev), (0, y_dev)):
        piece = item_slot(row, part)
        copy(piece, piece, ig_s.at[0], ig_r.at[4], device).start()
    for at, device in enumerate((x_dev, y_dev, p_dev)):
        copy(meta, metas.at[at], meta_s.at[0], meta_r.at[0], device).start()
    meta_x, meta_y, meta_p = metas.at[0], metas.at[1], metas.at[2]

    loads[2].wait()
    tile_t[...] = tile_v[...].reshape(size, size).T

    for part in range(2):
        arrived(item_slot(row_x, part, 4), ig_r.at[part])
        relay_item(row_x, part, 4, y_dev)
        arrived(item_slot(row_y, 2 + part, 4), ig_r.at[2 + part])
        relay_item(row_y, 2 + part, 4, x_dev)
    for at in near_first:
        slot = user_slot(2 * at + core)
        arrived(slot, uz_r.at[at])
        copy(slot, slot, up_s.at[0], up_r.at[0], p_dev).start()
    half_users = u_all.at[pl.ds(0, u_all.shape[0] // 2)]
    arrived(half_users, up_r.at[0])

    user_sel = u_all[tu]
    user_sel = jnp.where(live, user_sel, 0.0).astype(user_sel.dtype)
    product_i = jnp.dot(tile_t[...], user_sel, preferred_element_type=jnp.float32)
    part_i[...] = product_i.reshape(part_i.shape)
    code, peak = encode(product_i)
    peak_1[...] = peak
    send_1[...] = code.reshape(send_1.shape)
    for at, device in enumerate((x_dev, y_dev)):
        copy(peak_1, from_1p.at[at], r1p_s.at[0], r1p_r.at[at], device).start()
    for c in (0, 2, 1, 3):
        copy(
            send_1.at[c], from_1.at[c], r1_s.at[0], r1_r.at[c], x_dev if c < 2 else y_dev
        ).start()

    arrived(i_all.at[pl.ds(0, 2)], ig_r.at[4])
    item_sel = i_all[ti]
    item_sel = jnp.where(live, item_sel, 0.0).astype(item_sel.dtype)

    def multiply(owner):
        rows = jnp.concatenate([tile_v[2 * h + owner] for h in range(pieces)], axis=0)
        product = jnp.dot(rows, item_sel, preferred_element_type=jnp.float32)
        for h in range(pieces):
            part_u[2 * h + owner] = product[h * rows_u : (h + 1) * rows_u]

    multiply(1 - core)
    for h in range(pieces):
        copy(part_u.at[2 * h + 1 - core], from_p.at[h], rp_s.at[0], rp_r.at[0], p_dev).start()
    multiply(core)
    arrived(metas, meta_r.at[0])

    def second(c):
        other, owner, device = (
            (meta_x, row_y, y_dev) if c < 2 else (meta_y, row_x, x_dev)
        )
        theirs = other[1][0:1, :]
        arrived(from_1.at[c], r1_r.at[c])
        there = decode(from_1[c], from_1p[c // 2])
        send_2[c], peak_2[c] = encode(
            jnp.where(my_ti == owner, part_i[c], 0.0) + jnp.where(theirs == owner, there, 0.0)
        )
        copy(peak_2.at[c], from_2p.at[c], r2p_s.at[0], r2p_r.at[c], device).start()
        copy(send_2.at[c], from_2.at[c], r2_s.at[0], r2_r.at[c], device).start()

    partner_tu = meta_p[0][0:1, :]
    arrived(from_p, rp_r.at[0])
    for at, device in list(zip(others, z_devs)) + [(z, None)]:
        tile, h = at // pieces, at % pieces
        both = jnp.where(my_tu == tile, part_u[2 * h + core], 0.0) + jnp.where(
            partner_tu == tile, from_p[h], 0.0
        )
        if device is None:
            total = both
        else:
            send_z[at], peak_z[at] = encode(both)
            copy(peak_z.at[at], from_zp.at[z], rzp_s.at[0], rzp_r.at[0], device).start()
            copy(send_z.at[at], from_z.at[z], rz_s.at[0], rz_r.at[0], device).start()

    for at in range(2):
        arrived(from_1p.at[at], r1p_r.at[at])
    for c in (0, 2, 1, 3):
        second(c)

    for c in (0, 2, 1, 3):
        theirs = (meta_x if c < 2 else meta_y)[1][0:1, :]
        there = decode(from_1[c], from_1p[c // 2])
        mine = jnp.where(my_ti == row, part_i[c], 0.0) + jnp.where(theirs == row, there, 0.0)
        arrived(from_2p.at[c], r2p_r.at[c])
        arrived(from_2.at[c], r2_r.at[c])
        last = mine + decode(from_2[c], from_2p[c])
        out_i[pl.ds(c * chunk, chunk), :] = last.astype(out_i.dtype)

    arrived(from_zp.at[pl.ds(0, n_z - 1)], rzp_r.at[0])
    arrived(from_z.at[pl.ds(0, n_z - 1)], rz_r.at[0])
    for at in near_first:
        total = total + decode(from_z[at], from_zp[at])
    out_u[...] = total.astype(out_u.dtype)

    left(u_all.at[0, pl.ds(0, (n_z - 1) * rows_u)], uz_s.at[0])
    left(half_users, up_s.at[0])
    left(i_all.at[pl.ds(0, 3)], ig_s.at[0])
    left(metas, meta_s.at[0])
    left(send_1, r1_s.at[0])
    left(from_1p, r1p_s.at[0])
    left(from_p, rp_s.at[0])
    left(send_2, r2_s.at[0])
    left(peak_2, r2p_s.at[0])
    left(send_z.at[pl.ds(0, n_z - 1)], rz_s.at[0])
    left(peak_z.at[pl.ds(0, n_z - 1)], rzp_s.at[0])


def put(users, items, out_u, out_i, sems):
    copies = [
        pltpu.make_async_copy(users, out_u, sems.at[0]),
        pltpu.make_async_copy(items, out_i, sems.at[1]),
    ]
    for c in copies:
        c.start()
    for c in copies:
        c.wait()


def planned(user_feats, item_feats, tile_values, tile_coords, tile_count, *, n_z):
    rows_u, width = user_feats.shape
    rows_i = item_feats.shape[0]
    size = tile_values.shape[-1]
    f32, bf16, dma = jnp.float32, jnp.bfloat16, pltpu.SemaphoreType.DMA
    blocks = size // rows_u
    vmem = pl.BlockSpec(memory_space=pltpu.VMEM)
    anywhere = pl.BlockSpec(memory_space=pl.ANY)
    quarter = (4, rows_i // 4, width)
    arrivals = [1, n_z, 1, 5, 1, 1, 1, 4, 2, 4, 4]
    i16 = jnp.int16
    outs = pl.pallas_call(
        functools.partial(kernel, n_z),
        out_shape=(pltpu.VMEM((rows_u, width), bf16), pltpu.VMEM((rows_i, width), bf16)),
        in_specs=[anywhere] * 5,
        out_specs=(vmem, vmem),
        scratch_shapes=[
            pltpu.VMEM((2 * n_z * rows_u // size, size, width), bf16),
            pltpu.VMEM((4, rows_i, width), bf16),
            pltpu.VMEM((blocks, rows_u, size), bf16),
            pltpu.VMEM((size, size), bf16),
            pltpu.VMEM((3, 8, width), jnp.int32),
            pltpu.VMEM((3, 3, 8, width), jnp.int32),
            pltpu.VMEM((blocks, rows_u, width), f32),
            pltpu.VMEM((blocks // 2, rows_u, width), f32),
            pltpu.VMEM((n_z, rows_u, width), i16),
            pltpu.VMEM((n_z, 8, width), f32),
            pltpu.VMEM((n_z, rows_u, width), i16),
            pltpu.VMEM((n_z, 8, width), f32),
            pltpu.VMEM(quarter, f32),
            pltpu.VMEM(quarter, i16),
            pltpu.VMEM((8, width), f32),
            pltpu.VMEM(quarter, i16),
            pltpu.VMEM((2, 8, width), f32),
            pltpu.VMEM(quarter, i16),
            pltpu.VMEM((4, 8, width), f32),
            pltpu.VMEM(quarter, i16),
            pltpu.VMEM((4, 8, width), f32),
            pltpu.SMEM((2,), jnp.int32),
            pltpu.SMEM((1, 1), jnp.int32),
            dma((5,)),
        ]
        + [dma((n,)) for arrival in arrivals for n in (1, arrival)],
        compiler_params=pltpu.CompilerParams(collective_id=0, has_side_effects=True),
    )(
        tile_coords.reshape(2),
        tile_count,
        user_feats,
        item_feats,
        tile_values.reshape(blocks, rows_u, size),
    )
    return pl.pallas_call(
        put,
        out_shape=[jax.ShapeDtypeStruct(out.shape, out.dtype) for out in outs],
        in_specs=[vmem, vmem],
        out_specs=[anywhere, anywhere],
        scratch_shapes=[dma((2,))],
    )(*[pltpu.with_memory_space_constraint(out, pltpu.VMEM) for out in outs])


def solution(mesh):
    n_row, n_col = mesh.shape["row"], mesh.shape["col"]

    def local(user_feats, item_feats, tile_values, tile_coords, tile_count):
        slots, size = tile_values.shape[2], tile_values.shape[3]
        rows_u = user_feats.shape[0]
        fits = (
            n_row == 4
            and n_col % 2 == 0
            and slots == 1
            and item_feats.shape[0] == size
            and size % (2 * rows_u) == 0
            and n_col * rows_u % (2 * size) == 0
            and (n_col // 2 - 1) * rows_u <= size
        )
        args = (user_feats, item_feats, tile_values, tile_coords, tile_count)
        return planned(*args, n_z=n_col // 2) if fits else gathered(*args)

    placed = (
        P(("row", "col"), None),
        P(("col", "row"), None),
        P("row", "col", None, None, None),
        P("row", "col", None, None),
        P("row", "col"),
    )
    return jax.shard_map(
        local,
        mesh=mesh,
        in_specs=placed,
        out_specs=(P(("row", "col"), None), P(("col", "row"), None)),
        check_vma=False,
    )
```

```python
import functools
import math

import jax
import jax.numpy as jnp
from jax import lax
from jax.experimental import pallas as pl
from jax.experimental.pallas import tpu as pltpu
from jax.sharding import PartitionSpec as P

MESH = pl.DeviceIdType.MESH
STEPS = 32760.0
TINY = 1e-30


def gathered(user_feats, item_feats, tile_values, tile_coords, tile_count):
    user_block = lax.all_gather(user_feats, "col", axis=0, tiled=True)
    item_block = lax.all_gather(item_feats, "row", axis=0, tiled=True)
    tiles = tile_values[0, 0]
    coords = tile_coords[0, 0]
    count = tile_count[0, 0]
    slots = tiles.shape[0]
    size = tiles.shape[1]
    width = user_block.shape[1]
    user_tiles = user_block.shape[0] // size
    item_tiles = item_block.shape[0] // size
    live = jnp.arange(slots) < count
    pick_user = ((coords[0][:, None] == jnp.arange(user_tiles)[None, :]) & live[:, None]).astype(
        jnp.bfloat16
    )
    pick_item = (coords[1][:, None] == jnp.arange(item_tiles)[None, :]).astype(jnp.bfloat16)
    user_sel = jnp.einsum(
        "su,uiw->siw",
        pick_user,
        user_block.reshape(user_tiles, size, width),
        preferred_element_type=jnp.float32,
    ).astype(jnp.bfloat16)
    item_sel = jnp.einsum(
        "st,tjw->sjw",
        pick_item,
        item_block.reshape(item_tiles, size, width),
        preferred_element_type=jnp.float32,
    ).astype(jnp.bfloat16)
    to_users = jnp.einsum("sij,sjw->siw", tiles, item_sel, preferred_element_type=jnp.float32)
    to_items = jnp.einsum("sij,siw->sjw", tiles, user_sel, preferred_element_type=jnp.float32)
    part_users = jnp.einsum(
        "su,siw->uiw", pick_user.astype(jnp.float32), to_users, precision=lax.Precision.HIGHEST
    ).reshape(user_tiles * size, width)
    part_items = jnp.einsum(
        "st,sjw->tjw", pick_item.astype(jnp.float32), to_items, precision=lax.Precision.HIGHEST
    ).reshape(item_tiles * size, width)
    users_next = lax.psum_scatter(part_users, "col", scatter_dimension=0, tiled=True)
    items_next = lax.psum_scatter(part_items, "row", scatter_dimension=0, tiled=True)
    return (users_next.astype(jnp.bfloat16), items_next.astype(jnp.bfloat16))


def encode(values):
    rows, width = values.shape
    groups = values.reshape(rows // 8, 8, width)
    peak = jnp.maximum(jnp.max(jnp.abs(groups), axis=0), TINY)
    return encode_by(values, peak), peak


def encode_by(values, peak):
    rows, width = values.shape
    groups = values.reshape(rows // 8, 8, width)
    scaled = jnp.round(groups * (STEPS / peak)[None])
    return scaled.astype(jnp.int32).astype(jnp.int16).reshape(rows, width)


def decode(code, peak):
    rows, width = code.shape
    groups = code.astype(jnp.int32).astype(jnp.float32).reshape(rows // 8, 8, width)
    return (groups * (peak * (1.0 / STEPS))[None]).reshape(rows, width)


def kernel(
    n_z,
    coords_in,
    count_in,
    user_in,
    item_in,
    tile_in,
    out_u,
    out_i,
    u_all,
    i_got,
    r_own,
    r_near,
    s_sel,
    tile_v,
    tile_t,
    meta,
    metas,
    part_u,
    from_p,
    send_z,
    peak_z,
    from_z,
    from_zp,
    part_i,
    send_1,
    peak_1,
    from_1,
    from_1p,
    pair_1,
    pair_1p,
    fwd_1,
    mask_1p,
    fwd_1p,
    send_2,
    peak_2,
    from_2,
    from_2p,
    gauge,
    coords,
    count,
    load_sem,
    sent,
    meta_r,
    uz_r,
    up_r,
    io_r,
    iq_r,
    ig_r,
    rp_r,
    rz_r,
    r1_r,
    rq_r,
    rf_r,
    r2_r,
):
    row, col = lax.axis_index("row"), lax.axis_index("col")
    y, x = row // 2, row % 2
    z, core = col // 2, col % 2
    row_x, row_y = 2 * y + 1 - x, 2 * (1 - y) + x
    twin = 2 * z + 1 - core
    x_dev, y_dev, p_dev = (row_x, twin), (row_y, twin), (row, twin)
    high = z // (n_z // 2)

    def far_first(at):
        mirrored = z + high * (n_z - 1 - 2 * z)
        to = n_z - 1 - at
        to = jnp.where(to <= mirrored, to - 1, to)
        return to + high * (n_z - 1 - 2 * to)

    others = [far_first(at) for at in range(n_z - 1)]
    z_devs = [(row, 2 * at + 1 - core) for at in others]
    near_first = others[::-1]
    rows_u, rows_i = user_in.shape[0], i_got.shape[0] * i_got.shape[2]
    size = tile_v.shape[-1]
    width = user_in.shape[1]
    half, chunk = rows_i // 2, rows_i // 4
    pieces = size // rows_u // 2
    order = (0, 2, 1, 3)
    sizes = []

    def user_slot(at):
        blocks = size // rows_u
        inner = pl.multiple_of(at % blocks * rows_u, rows_u)
        return u_all.at[at // blocks, pl.ds(inner, rows_u)]

    def quarter(c):
        return pl.ds(c % 2 * chunk, chunk)

    def send(src, dst, recv, device):
        sizes.append(math.prod(src.shape) * src.dtype.itemsize)
        copy(src, dst, sent.at[0], recv, device).start()

    def copy(src, dst, sem, recv, device):
        return pltpu.make_async_remote_copy(
            src_ref=src,
            dst_ref=dst,
            send_sem=sem,
            recv_sem=recv,
            device_id=device,
            device_id_type=MESH,
        )

    def arrived(like, recv):
        copy(like, like, recv, recv, x_dev).wait_recv()

    def landed(recv, *likes):
        total = sum(math.prod(like.shape) * like.dtype.itemsize for like in likes)
        arrived(gauge.at[pl.ds(0, total // (4 * width))], recv)

    barrier = pltpu.get_barrier_semaphore()
    peers = [x_dev, y_dev, p_dev] + z_devs
    for peer in peers:
        pl.semaphore_signal(barrier, inc=1, device_id=peer, device_id_type=MESH)
    loads = [
        pltpu.make_async_copy(user_in, user_slot(col), load_sem.at[0]),
        pltpu.make_async_copy(item_in, i_got.at[:, 0], load_sem.at[1]),
        pltpu.make_async_copy(tile_in, tile_v, load_sem.at[2]),
        pltpu.make_async_copy(coords_in, coords, load_sem.at[3]),
        pltpu.make_async_copy(count_in, count, load_sem.at[4]),
    ]
    for load in loads:
        load.start()

    loads[3].wait()
    loads[4].wait()
    tu, ti = coords[0], coords[1]
    meta[0] = jnp.full(meta.shape[1:], tu, jnp.int32)
    meta[1] = jnp.full(meta.shape[1:], ti, jnp.int32)
    my_tu, my_ti = meta[0][0:1, :], meta[1][0:1, :]
    live = jnp.full((1, width), count[0, 0], jnp.int32) > 0
    pl.semaphore_wait(barrier, len(peers))

    loads[0].wait()
    own = user_slot(col)
    for device in z_devs:
        send(own, own, uz_r.at[z], device)
    for at, device in enumerate((x_dev, y_dev, p_dev)):
        send(meta, metas.at[at], meta_r.at[0], device)
    loads[1].wait()
    for c in order:
        send(
            i_got.at[c // 2, 0, quarter(c)],
            r_near.at[c // 2, quarter(c)],
            iq_r.at[c],
            x_dev if c < 2 else y_dev,
        )
    send(own, own, up_r.at[0], p_dev)
    for part in range(2):
        send(i_got.at[part, 0], r_own.at[part], io_r.at[0], p_dev)

    loads[2].wait()
    tile_t[...] = tile_v[...].reshape(size, size).T
    arrived(metas, meta_r.at[0])
    x_ti, y_ti, p_ti = (metas[at, 1][0:1, :] for at in range(3))
    p_tu = metas[2, 0][0:1, :]
    arrived(r_own, io_r.at[0])

    def pass_user(at):
        slot = user_slot(2 * at + 1 - core)
        arrived(slot, uz_r.at[at])
        copy(slot, slot, sent.at[0], up_r.at[0], p_dev).start()

    def pass_items(c):
        part, want, near, device = (
            (0, y_ti, row_x, y_dev) if c < 2 else (1, x_ti, row_y, x_dev)
        )
        here = r_near.at[part, quarter(c)]
        arrived(here, iq_r.at[c])
        s_sel[part, quarter(c)] = jnp.where(
            want == near, r_near[part, quarter(c)], r_own[part, quarter(c)]
        )
        copy(
            s_sel.at[part, quarter(c)],
            i_got.at[part, 2, quarter(c)],
            sent.at[0],
            ig_r.at[0],
            device,
        ).start()
        copy(here, i_got.at[part, 1, quarter(c)], sent.at[0], ig_r.at[0], p_dev).start()

    users = [(pass_user, at) for at in near_first]
    items = [(pass_items, c) for c in order]
    sizes.extend([rows_u * width * 2] * len(users) + [chunk * width * 2] * (2 * len(items)))

    for step, at in users[:-1] + items + users[-1:]:
        step(at)

    arrived(u_all.at[pl.ds(0, u_all.shape[0] // 2)], up_r.at[0])

    user_sel = u_all[tu]
    user_sel = jnp.where(live, user_sel, 0.0).astype(user_sel.dtype)
    product_i = jnp.dot(tile_t[...], user_sel, preferred_element_type=jnp.float32)
    code, peak = encode(product_i)
    peak_1[...] = peak
    send_1[...] = code.reshape(send_1.shape)
    for at, device in enumerate((x_dev, y_dev)):
        send(peak_1, from_1p.at[at], r1_r.at[2 * at], device)
    for c in order:
        send(send_1.at[c], from_1.at[c], r1_r.at[c], x_dev if c < 2 else y_dev)
    send(peak_1, pair_1p, rq_r.at[0], p_dev)
    send(send_1, pair_1, rq_r.at[0], p_dev)
    part_i[...] = product_i.reshape(part_i.shape)

    arrived(i_got.at[:, pl.ds(1, 2)], ig_r.at[0])
    sel_x = jnp.where(ti == row, 0, jnp.where(ti == row_x, 1, 2))
    sel_y = jnp.where(ti == row, 0, jnp.where(ti == row_y, 1, 2))
    item_sel = jnp.concatenate([i_got[0, sel_x], i_got[1, sel_y]], axis=0)
    item_sel = jnp.where(live, item_sel, 0.0).astype(item_sel.dtype)

    def multiply(owner):
        rows = jnp.concatenate([tile_v[2 * h + owner] for h in range(pieces)], axis=0)
        product = jnp.dot(rows, item_sel, preferred_element_type=jnp.float32)
        for h in range(pieces):
            part_u[2 * h + owner] = product[h * rows_u : (h + 1) * rows_u]

    multiply(core)
    for h in range(pieces):
        send(part_u.at[2 * h + core], from_p.at[h], rp_r.at[0], p_dev)
    multiply(1 - core)

    def users_out():
        arrived(from_p, rp_r.at[0])
        for at, device in list(zip(others, z_devs)) + [(z, p_dev)]:
            tile, h = at // pieces, at % pieces
            send_z[at], peak_z[at] = encode(
                jnp.where(my_tu == tile, part_u[2 * h + 1 - core], 0.0)
                + jnp.where(p_tu == tile, from_p[h], 0.0)
            )
            copy(peak_z.at[at], from_zp.at[z], sent.at[0], rz_r.at[0], device).start()
            copy(send_z.at[at], from_z.at[z], sent.at[0], rz_r.at[0], device).start()

    def items_out():
        landed(rq_r.at[0], pair_1, pair_1p)
        for c in order:
            other, owner, device = (
                (x_ti, row_y, y_dev) if c < 2 else (y_ti, row_x, x_dev)
            )
            at = c // 2
            if c % 2 == 0:
                landed(r1_r.at[c], from_1.at[c], peak_1)
                mask_1p[at] = jnp.where(other == row, from_1p[at], 0.0)
                copy(mask_1p.at[at], fwd_1p.at[at], sent.at[0], rf_r.at[0], p_dev).start()
            else:
                arrived(from_1.at[c], r1_r.at[c])
            send_2[c], peak_2[c] = encode(
                jnp.where(p_ti == owner, decode(pair_1[c], pair_1p[...]), 0.0)
                + jnp.where(other == owner, decode(from_1[c], from_1p[at]), 0.0)
            )
            copy(peak_2.at[c], from_2p.at[c], sent.at[0], r2_r.at[c % 2], device).start()
            copy(send_2.at[c], from_2.at[c], sent.at[0], r2_r.at[c % 2], device).start()
            copy(from_1.at[c], fwd_1.at[c], sent.at[0], rf_r.at[0], p_dev).start()

    for ref in (peak_z, send_z, mask_1p, peak_2, send_2, from_1):
        sizes.append(math.prod(ref.shape) * ref.dtype.itemsize)

    users_out()
    items_out()

    landed(rf_r.at[0], fwd_1, fwd_1p)
    for c in order:
        if c in (0, 1):
            landed(r2_r.at[c % 2], from_2.at[pl.ds(0, 2)], from_2p.at[pl.ds(0, 2)])
        last = jnp.where(my_ti == row, part_i[c], 0.0) + decode(fwd_1[c], fwd_1p[c // 2])
        last = last + decode(from_2[c], from_2p[c])
        out_i[pl.ds(c * chunk, chunk), :] = last.astype(out_i.dtype)

    landed(rz_r.at[0], from_z, from_zp)
    total = decode(from_z[0], from_zp[0])
    for at in range(1, n_z):
        total = total + decode(from_z[at], from_zp[at])
    out_u[...] = total.astype(out_u.dtype)

    like = gauge.at[pl.ds(0, sum(sizes) // (4 * width))]
    copy(like, like, sent.at[0], sent.at[0], x_dev).wait_send()


def put(users, items, out_u, out_i, sems):
    copies = [
        pltpu.make_async_copy(users, out_u, sems.at[0]),
        pltpu.make_async_copy(items, out_i, sems.at[1]),
    ]
    for c in copies:
        c.start()
    for c in copies:
        c.wait()


def planned(user_feats, item_feats, tile_values, tile_coords, tile_count, *, n_z):
    rows_u, width = user_feats.shape
    rows_i = item_feats.shape[0]
    size = tile_values.shape[-1]
    f32, bf16, dma = jnp.float32, jnp.bfloat16, pltpu.SemaphoreType.DMA
    blocks = size // rows_u
    vmem = pl.BlockSpec(memory_space=pltpu.VMEM)
    anywhere = pl.BlockSpec(memory_space=pl.ANY)
    quarter = (4, rows_i // 4, width)
    peak = (8, width)
    i16 = jnp.int16
    vm = pltpu.VMEM
    outs = pl.pallas_call(
        functools.partial(kernel, n_z),
        out_shape=(pltpu.VMEM((rows_u, width), bf16), pltpu.VMEM((rows_i, width), bf16)),
        in_specs=[anywhere] * 5,
        out_specs=(vmem, vmem),
        scratch_shapes=[
            vm((2 * n_z * rows_u // size, size, width), bf16),
            vm((2, 3, rows_i // 2, width), bf16),
            vm((2, rows_i // 2, width), bf16),
            vm((2, rows_i // 2, width), bf16),
            vm((2, rows_i // 2, width), bf16),
            vm((blocks, rows_u, size), bf16),
            vm((size, size), bf16),
            vm((2,) + peak, jnp.int32),
            vm((3, 2) + peak, jnp.int32),
            vm((blocks, rows_u, width), f32),
            vm((blocks // 2, rows_u, width), f32),
            vm((n_z, rows_u, width), i16),
            vm((n_z,) + peak, f32),
            vm((n_z, rows_u, width), i16),
            vm((n_z,) + peak, f32),
            vm(quarter, f32),
            vm(quarter, i16),
            vm(peak, f32),
            vm(quarter, i16),
            vm((2,) + peak, f32),
            vm(quarter, i16),
            vm(peak, f32),
            vm(quarter, i16),
            vm((2,) + peak, f32),
            vm((2,) + peak, f32),
            vm(quarter, i16),
            vm((4,) + peak, f32),
            vm(quarter, i16),
            vm((4,) + peak, f32),
            vm((16 * rows_i, width), f32),
            pltpu.SMEM((2,), jnp.int32),
            pltpu.SMEM((1, 1), jnp.int32),
        ]
        + [dma((n,)) for n in (5, 1, 1, n_z, 1, 1, 4, 1, 1, 1, 4, 1, 1, 2)],
        compiler_params=pltpu.CompilerParams(collective_id=0, has_side_effects=True),
    )(
        tile_coords.reshape(2),
        tile_count,
        user_feats,
        item_feats.reshape(2, rows_i // 2, width),
        tile_values.reshape(blocks, rows_u, size),
    )
    return pl.pallas_call(
        put,
        out_shape=[jax.ShapeDtypeStruct(out.shape, out.dtype) for out in outs],
        in_specs=[vmem, vmem],
        out_specs=[anywhere, anywhere],
        scratch_shapes=[dma((2,))],
    )(*[pltpu.with_memory_space_constraint(out, pltpu.VMEM) for out in outs])


def solution(mesh):
    n_row, n_col = mesh.shape["row"], mesh.shape["col"]

    def local(user_feats, item_feats, tile_values, tile_coords, tile_count):
        slots, size = tile_values.shape[2], tile_values.shape[3]
        rows_u = user_feats.shape[0]
        fits = (
            n_row == 4
            and n_col % 2 == 0
            and slots == 1
            and item_feats.shape[0] == size
            and size % (2 * rows_u) == 0
            and n_col * rows_u % (2 * size) == 0
            and (n_col // 2 - 1) * rows_u <= size
        )
        args = (user_feats, item_feats, tile_values, tile_coords, tile_count)
        return planned(*args, n_z=n_col // 2) if fits else gathered(*args)

    placed = (
        P(("row", "col"), None),
        P(("col", "row"), None),
        P("row", "col", None, None, None),
        P("row", "col", None, None),
        P("row", "col"),
    )
    return jax.shard_map(
        local,
        mesh=mesh,
        in_specs=placed,
        out_specs=(P(("row", "col"), None), P(("col", "row"), None)),
        check_vma=False,
    )
```

```python
import functools
import math

import jax
import jax.numpy as jnp
from jax import lax
from jax.experimental import pallas as pl
from jax.experimental.pallas import tpu as pltpu
from jax.sharding import PartitionSpec as P

MESH = pl.DeviceIdType.MESH
LEVELS = 32760.0
STEPS = 4
TINY = 1e-30


def gathered(user_feats, item_feats, tile_values, tile_coords, tile_count):
    user_block = lax.all_gather(user_feats, "col", axis=0, tiled=True)
    item_block = lax.all_gather(item_feats, "row", axis=0, tiled=True)
    tiles = tile_values[0, 0]
    coords = tile_coords[0, 0]
    count = tile_count[0, 0]
    slots = tiles.shape[0]
    size = tiles.shape[1]
    width = user_block.shape[1]
    user_tiles = user_block.shape[0] // size
    item_tiles = item_block.shape[0] // size
    live = jnp.arange(slots) < count
    pick_user = ((coords[0][:, None] == jnp.arange(user_tiles)[None, :]) & live[:, None]).astype(
        jnp.bfloat16
    )
    pick_item = (coords[1][:, None] == jnp.arange(item_tiles)[None, :]).astype(jnp.bfloat16)
    user_sel = jnp.einsum(
        "su,uiw->siw",
        pick_user,
        user_block.reshape(user_tiles, size, width),
        preferred_element_type=jnp.float32,
    ).astype(jnp.bfloat16)
    item_sel = jnp.einsum(
        "st,tjw->sjw",
        pick_item,
        item_block.reshape(item_tiles, size, width),
        preferred_element_type=jnp.float32,
    ).astype(jnp.bfloat16)
    to_users = jnp.einsum("sij,sjw->siw", tiles, item_sel, preferred_element_type=jnp.float32)
    to_items = jnp.einsum("sij,siw->sjw", tiles, user_sel, preferred_element_type=jnp.float32)
    part_users = jnp.einsum(
        "su,siw->uiw", pick_user.astype(jnp.float32), to_users, precision=lax.Precision.HIGHEST
    ).reshape(user_tiles * size, width)
    part_items = jnp.einsum(
        "st,sjw->tjw", pick_item.astype(jnp.float32), to_items, precision=lax.Precision.HIGHEST
    ).reshape(item_tiles * size, width)
    users_next = lax.psum_scatter(part_users, "col", scatter_dimension=0, tiled=True)
    items_next = lax.psum_scatter(part_items, "row", scatter_dimension=0, tiled=True)
    return (users_next.astype(jnp.bfloat16), items_next.astype(jnp.bfloat16))


def encode(values):
    rows, width = values.shape
    groups = values.reshape(rows // 8, 8, width)
    peak = jnp.maximum(jnp.max(jnp.abs(groups), axis=0), TINY)
    return encode_by(values, peak), peak


def encode_by(values, peak):
    rows, width = values.shape
    groups = values.reshape(rows // 8, 8, width)
    scaled = jnp.round(groups * (LEVELS / peak)[None])
    return scaled.astype(jnp.int32).astype(jnp.int16).reshape(rows, width)


def decode(code, peak):
    rows, width = code.shape
    groups = code.astype(jnp.int32).astype(jnp.float32).reshape(rows // 8, 8, width)
    return (groups * (peak * (1.0 / LEVELS))[None]).reshape(rows, width)


def kernel(
    n_z,
    coords_in,
    count_in,
    user_in,
    item_in,
    tile_in,
    out_u,
    out_i,
    u_all,
    i_got,
    r_own,
    r_near,
    s_sel,
    tile_v,
    tile_t,
    meta,
    metas,
    part_u,
    from_p,
    send_z,
    peak_z,
    from_z,
    from_zp,
    part_i,
    send_1,
    peak_1,
    from_1,
    from_1p,
    pair_1,
    pair_1p,
    fwd_1,
    mask_1p,
    fwd_1p,
    send_2,
    peak_2,
    from_2,
    from_2p,
    gauge,
    coords,
    count,
    load_sem,
    sent,
    first_s,
    late,
    meta_r,
    uz_r,
    up_r,
    io_r,
    iq_r,
    ig_r,
    rp_r,
    rz_r,
    r1_r,
    rq_r,
    rf_r,
    r2_r,
):
    row, col = lax.axis_index("row"), lax.axis_index("col")
    y, x = row // 2, row % 2
    z, core = col // 2, col % 2
    row_x, row_y = 2 * y + 1 - x, 2 * (1 - y) + x
    twin = 2 * z + 1 - core
    x_dev, y_dev, p_dev = (row_x, twin), (row_y, twin), (row, twin)
    high = z // (n_z // 2)

    def far_first(at):
        mirrored = z + high * (n_z - 1 - 2 * z)
        to = n_z - 1 - at
        to = jnp.where(to <= mirrored, to - 1, to)
        return to + high * (n_z - 1 - 2 * to)

    others = [far_first(at) for at in range(n_z - 1)]
    z_devs = [(row, 2 * at + 1 - core) for at in others]
    near_first = others[::-1]
    rows_u, rows_i = user_in.shape[0], i_got.shape[0] * i_got.shape[2]
    size = tile_v.shape[-1]
    width = user_in.shape[1]
    steps = send_1.shape[1]
    chunk = rows_i // (2 * steps)
    pieces = size // rows_u // 2
    sizes = []

    def user_slot(at):
        blocks = size // rows_u
        inner = pl.multiple_of(at % blocks * rows_u, rows_u)
        return u_all.at[at // blocks, pl.ds(inner, rows_u)]

    def rows_of(step):
        return pl.ds(step * chunk, chunk)

    def send(src, dst, recv, device):
        sizes.append(math.prod(src.shape) * src.dtype.itemsize)
        copy(src, dst, sent.at[0], recv, device).start()

    def copy(src, dst, sem, recv, device):
        return pltpu.make_async_remote_copy(
            src_ref=src,
            dst_ref=dst,
            send_sem=sem,
            recv_sem=recv,
            device_id=device,
            device_id_type=MESH,
        )

    def arrived(like, recv):
        copy(like, like, recv, recv, x_dev).wait_recv()

    def landed(recv, *likes):
        total = sum(math.prod(like.shape) * like.dtype.itemsize for like in likes)
        arrived(gauge.at[pl.ds(0, total // (4 * width))], recv)

    barrier = pltpu.get_barrier_semaphore()
    across, mates = z_devs[: n_z // 2], z_devs[n_z // 2 :]
    peers = [x_dev, y_dev, p_dev] + mates
    for peer in peers:
        pl.semaphore_signal(barrier, inc=1, device_id=peer, device_id_type=MESH)

    @pl.when(high == 0)
    def _():
        for peer in across:
            pl.semaphore_signal(barrier, inc=1, device_id=peer, device_id_type=MESH)

    loads = [
        pltpu.make_async_copy(user_in, user_slot(col), load_sem.at[0]),
        pltpu.make_async_copy(item_in, i_got.at[:, 0], load_sem.at[1]),
        pltpu.make_async_copy(tile_in, tile_v, load_sem.at[2]),
        pltpu.make_async_copy(coords_in, coords, load_sem.at[3]),
        pltpu.make_async_copy(count_in, count, load_sem.at[4]),
    ]
    for load in loads:
        load.start()

    loads[3].wait()
    loads[4].wait()
    tu, ti = coords[0], coords[1]
    meta[0] = jnp.full(meta.shape[1:], tu, jnp.int32)
    meta[1] = jnp.full(meta.shape[1:], ti, jnp.int32)
    my_tu, my_ti = meta[0][0:1, :], meta[1][0:1, :]
    live = jnp.full((1, width), count[0, 0], jnp.int32) > 0
    pl.semaphore_wait(barrier, len(peers) + high * len(across))

    loads[0].wait()
    own = user_slot(col)

    @pl.when(high == 1)
    def _():
        for peer in across:
            pl.semaphore_signal(late, inc=1, device_id=peer, device_id_type=MESH)
        copy(own, own, first_s.at[0], uz_r.at[z], across[0]).start()

    sizes.extend([rows_u * width * 2] * (len(across) - 1))
    for device in mates:
        send(own, own, uz_r.at[z], device)
    for at, device in enumerate((x_dev, y_dev, p_dev)):
        send(meta, metas.at[at], meta_r.at[0], device)
    loads[1].wait()
    for step in range(steps):
        for part, device in ((0, x_dev), (1, y_dev)):
            send(
                i_got.at[part, 0, rows_of(step)],
                r_near.at[part, rows_of(step)],
                iq_r.at[step],
                device,
            )
    send(own, own, up_r.at[0], p_dev)
    for part in range(2):
        send(i_got.at[part, 0], r_own.at[part], io_r.at[0], p_dev)

    loads[2].wait()
    tile_t[...] = tile_v[...].reshape(size, size).T
    @pl.when(high == 1)
    def _():
        copy(own, own, first_s.at[0], uz_r.at[z], across[0]).wait_send()
        for device in across[1:]:
            copy(own, own, sent.at[0], uz_r.at[z], device).start()

    arrived(metas, meta_r.at[0])
    x_ti, y_ti, p_ti = (metas[at, 1][0:1, :] for at in range(3))
    p_tu = metas[2, 0][0:1, :]
    arrived(r_own, io_r.at[0])

    def pass_user(at):
        slot = user_slot(2 * at + 1 - core)
        arrived(slot, uz_r.at[at])
        copy(slot, slot, sent.at[0], up_r.at[0], p_dev).start()

    def pass_items(step):
        landed(iq_r.at[step], r_near.at[:, rows_of(step)])
        for part, want, near, device in ((0, y_ti, row_x, y_dev), (1, x_ti, row_y, x_dev)):
            here = (part, rows_of(step))
            s_sel[here] = jnp.where(want == near, r_near[here], r_own[here])
            copy(
                s_sel.at[here], i_got.at[part, 2, rows_of(step)], sent.at[0], ig_r.at[0], device
            ).start()
            copy(
                r_near.at[here], i_got.at[part, 1, rows_of(step)], sent.at[0], ig_r.at[0], p_dev
            ).start()

    users = [(pass_user, at) for at in near_first]
    items = [(pass_items, step) for step in range(steps)]
    sizes.extend([rows_u * width * 2] * len(users) + [chunk * width * 2] * (4 * steps))

    for step, at in users[: len(mates)]:
        step(at)

    @pl.when(high == 0)
    def _():
        pl.semaphore_wait(late, len(across))
        for device in across[:0:-1]:
            copy(own, own, sent.at[0], uz_r.at[z], device).start()
        copy(own, own, first_s.at[0], uz_r.at[z], across[0]).start()

    for step, at in items + users[len(mates) :]:
        step(at)

    def users_product():
        arrived(i_got.at[:, pl.ds(1, 2)], ig_r.at[0])
        sel_x = jnp.where(ti == row, 0, jnp.where(ti == row_x, 1, 2))
        sel_y = jnp.where(ti == row, 0, jnp.where(ti == row_y, 1, 2))
        item_sel = jnp.concatenate([i_got[0, sel_x], i_got[1, sel_y]], axis=0)
        item_sel = jnp.where(live, item_sel, 0.0).astype(item_sel.dtype)

        def multiply(owner):
            rows = jnp.concatenate([tile_v[2 * h + owner] for h in range(pieces)], axis=0)
            product = jnp.dot(rows, item_sel, preferred_element_type=jnp.float32)
            for h in range(pieces):
                part_u[2 * h + owner] = product[h * rows_u : (h + 1) * rows_u]

        multiply(core)
        for h in range(pieces):
            copy(part_u.at[2 * h + core], from_p.at[h], sent.at[0], rp_r.at[0], p_dev).start()
        multiply(1 - core)

    def items_product():
        arrived(u_all.at[pl.ds(0, u_all.shape[0] // 2)], up_r.at[0])

        user_sel = u_all[tu]
        user_sel = jnp.where(live, user_sel, 0.0).astype(user_sel.dtype)
        product_i = jnp.dot(tile_t[...], user_sel, preferred_element_type=jnp.float32)
        code, peak = encode(product_i)
        peak_1[...] = peak
        send_1[...] = code.reshape(send_1.shape)
        for part, device in enumerate((x_dev, y_dev)):
            copy(peak_1, from_1p.at[part], sent.at[0], r1_r.at[0], device).start()
        for step in range(steps):
            for part, device in enumerate((x_dev, y_dev)):
                here = (part, step)
                copy(send_1.at[here], from_1.at[here], sent.at[0], r1_r.at[step], device).start()
        copy(peak_1, pair_1p, sent.at[0], rq_r.at[0], p_dev).start()
        copy(send_1, pair_1, sent.at[0], rq_r.at[0], p_dev).start()
        part_i[...] = product_i.reshape(part_i.shape)

    for ref in (from_p, peak_1, peak_1, peak_1, send_1, send_1):
        sizes.append(math.prod(ref.shape) * ref.dtype.itemsize)

    @pl.when(high == 0)
    def _():
        items_product()
        users_product()

    @pl.when(high == 1)
    def _():
        users_product()
        items_product()

    def users_out():
        arrived(from_p, rp_r.at[0])
        for at, device in list(zip(others, z_devs)) + [(z, p_dev)]:
            tile, h = at // pieces, at % pieces
            send_z[at], peak_z[at] = encode(
                jnp.where(my_tu == tile, part_u[2 * h + 1 - core], 0.0)
                + jnp.where(p_tu == tile, from_p[h], 0.0)
            )
            copy(peak_z.at[at], from_zp.at[z], sent.at[0], rz_r.at[0], device).start()
            copy(send_z.at[at], from_z.at[z], sent.at[0], rz_r.at[0], device).start()

    def items_out():
        landed(rq_r.at[0], pair_1, pair_1p)
        sides = ((0, x_ti, row_y, y_dev), (1, y_ti, row_x, x_dev))
        for step in range(steps):
            if step == 0:
                landed(r1_r.at[0], from_1.at[:, 0], from_1p)
                for part, other, owner, device in sides:
                    mask_1p[part] = jnp.where(other == row, from_1p[part], 0.0)
                    peak_2[part] = jnp.where(p_ti == owner, pair_1p[...], 0.0) + jnp.where(
                        other == owner, from_1p[part], TINY
                    )
                    copy(
                        peak_2.at[part], from_2p.at[part], sent.at[0], r2_r.at[0], device
                    ).start()
            else:
                landed(r1_r.at[step], from_1.at[:, step])
            for part, other, owner, device in sides:
                here = (part, step)
                send_2[here] = encode_by(
                    jnp.where(p_ti == owner, decode(pair_1[here], pair_1p[...]), 0.0)
                    + jnp.where(other == owner, decode(from_1[here], from_1p[part]), 0.0),
                    peak_2[part],
                )
                copy(
                    send_2.at[here], from_2.at[here], sent.at[0], r2_r.at[step], device
                ).start()
            for part in range(2):
                here = (part, step)
                copy(from_1.at[here], fwd_1.at[here], sent.at[0], rf_r.at[0], p_dev).start()
        copy(mask_1p, fwd_1p, sent.at[0], rf_r.at[0], p_dev).start()

    for ref in (peak_z, send_z, mask_1p, peak_2, send_2, from_1):
        sizes.append(math.prod(ref.shape) * ref.dtype.itemsize)

    users_out()
    items_out()

    landed(rf_r.at[0], fwd_1, fwd_1p)
    for step in range(steps):
        if step == 0:
            landed(r2_r.at[0], from_2.at[:, 0], from_2p)
        else:
            landed(r2_r.at[step], from_2.at[:, step])
        for part in range(2):
            here = (part, step)
            last = jnp.where(my_ti == row, part_i[here], 0.0)
            last = last + decode(fwd_1[here], fwd_1p[part])
            last = last + decode(from_2[here], from_2p[part])
            start = part * (rows_i // 2) + step * chunk
            out_i[pl.ds(start, chunk), :] = last.astype(out_i.dtype)

    landed(rz_r.at[0], from_z, from_zp)
    total = decode(from_z[0], from_zp[0])
    for at in range(1, n_z):
        total = total + decode(from_z[at], from_zp[at])
    out_u[...] = total.astype(out_u.dtype)

    @pl.when(high == 0)
    def _():
        copy(own, own, first_s.at[0], uz_r.at[z], across[0]).wait_send()

    like = gauge.at[pl.ds(0, sum(sizes) // (4 * width))]
    copy(like, like, sent.at[0], sent.at[0], x_dev).wait_send()


def put(users, items, out_u, out_i, sems):
    copies = [
        pltpu.make_async_copy(users, out_u, sems.at[0]),
        pltpu.make_async_copy(items, out_i, sems.at[1]),
    ]
    for c in copies:
        c.start()
    for c in copies:
        c.wait()


def planned(user_feats, item_feats, tile_values, tile_coords, tile_count, *, n_z):
    rows_u, width = user_feats.shape
    rows_i = item_feats.shape[0]
    size = tile_values.shape[-1]
    f32, bf16, dma = jnp.float32, jnp.bfloat16, pltpu.SemaphoreType.DMA
    blocks = size // rows_u
    vmem = pl.BlockSpec(memory_space=pltpu.VMEM)
    anywhere = pl.BlockSpec(memory_space=pl.ANY)
    cut = (2, STEPS, rows_i // (2 * STEPS), width)
    peak = (8, width)
    i16 = jnp.int16
    vm = pltpu.VMEM
    outs = pl.pallas_call(
        functools.partial(kernel, n_z),
        out_shape=(pltpu.VMEM((rows_u, width), bf16), pltpu.VMEM((rows_i, width), bf16)),
        in_specs=[anywhere] * 5,
        out_specs=(vmem, vmem),
        scratch_shapes=[
            vm((2 * n_z * rows_u // size, size, width), bf16),
            vm((2, 3, rows_i // 2, width), bf16),
            vm((2, rows_i // 2, width), bf16),
            vm((2, rows_i // 2, width), bf16),
            vm((2, rows_i // 2, width), bf16),
            vm((blocks, rows_u, size), bf16),
            vm((size, size), bf16),
            vm((2,) + peak, jnp.int32),
            vm((3, 2) + peak, jnp.int32),
            vm((blocks, rows_u, width), f32),
            vm((blocks // 2, rows_u, width), f32),
            vm((n_z, rows_u, width), i16),
            vm((n_z,) + peak, f32),
            vm((n_z, rows_u, width), i16),
            vm((n_z,) + peak, f32),
            vm(cut, f32),
            vm(cut, i16),
            vm(peak, f32),
            vm(cut, i16),
            vm((2,) + peak, f32),
            vm(cut, i16),
            vm(peak, f32),
            vm(cut, i16),
            vm((2,) + peak, f32),
            vm((2,) + peak, f32),
            vm(cut, i16),
            vm((2,) + peak, f32),
            vm(cut, i16),
            vm((2,) + peak, f32),
            vm((16 * rows_i, width), f32),
            pltpu.SMEM((2,), jnp.int32),
            pltpu.SMEM((1, 1), jnp.int32),
        ]
        + [dma((n,)) for n in (5, 1, 1)]
        + [pltpu.SemaphoreType.REGULAR]
        + [dma((n,)) for n in (1, n_z, 1, 1, STEPS, 1, 1, 1, STEPS, 1, 1, STEPS)],
        compiler_params=pltpu.CompilerParams(collective_id=0, has_side_effects=True),
    )(
        tile_coords.reshape(2),
        tile_count,
        user_feats,
        item_feats.reshape(2, rows_i // 2, width),
        tile_values.reshape(blocks, rows_u, size),
    )
    return pl.pallas_call(
        put,
        out_shape=[jax.ShapeDtypeStruct(out.shape, out.dtype) for out in outs],
        in_specs=[vmem, vmem],
        out_specs=[anywhere, anywhere],
        scratch_shapes=[dma((2,))],
    )(*[pltpu.with_memory_space_constraint(out, pltpu.VMEM) for out in outs])


def solution(mesh):
    n_row, n_col = mesh.shape["row"], mesh.shape["col"]

    def local(user_feats, item_feats, tile_values, tile_coords, tile_count):
        slots, size = tile_values.shape[2], tile_values.shape[3]
        rows_u = user_feats.shape[0]
        fits = (
            n_row == 4
            and n_col % 2 == 0
            and slots == 1
            and item_feats.shape[0] == size
            and size % (2 * rows_u) == 0
            and size % (32 * STEPS) == 0
            and n_col * rows_u % (2 * size) == 0
            and (n_col // 2 - 1) * rows_u <= size
        )
        args = (user_feats, item_feats, tile_values, tile_coords, tile_count)
        return planned(*args, n_z=n_col // 2) if fits else gathered(*args)

    placed = (
        P(("row", "col"), None),
        P(("col", "row"), None),
        P("row", "col", None, None, None),
        P("row", "col", None, None),
        P("row", "col"),
    )
    return jax.shard_map(
        local,
        mesh=mesh,
        in_specs=placed,
        out_specs=(P(("row", "col"), None), P(("col", "row"), None)),
        check_vma=False,
    )
```

```python
import functools
import math

import jax
import jax.numpy as jnp
from jax import lax
from jax.experimental import pallas as pl
from jax.experimental.pallas import tpu as pltpu
from jax.sharding import PartitionSpec as P

MESH = pl.DeviceIdType.MESH
LEVELS = 32760.0
STEPS = 4
GROUPS = 2
TINY = 1e-30


def gathered(user_feats, item_feats, tile_values, tile_coords, tile_count):
    user_block = lax.all_gather(user_feats, "col", axis=0, tiled=True)
    item_block = lax.all_gather(item_feats, "row", axis=0, tiled=True)
    tiles = tile_values[0, 0]
    coords = tile_coords[0, 0]
    count = tile_count[0, 0]
    slots = tiles.shape[0]
    size = tiles.shape[1]
    width = user_block.shape[1]
    user_tiles = user_block.shape[0] // size
    item_tiles = item_block.shape[0] // size
    live = jnp.arange(slots) < count
    pick_user = ((coords[0][:, None] == jnp.arange(user_tiles)[None, :]) & live[:, None]).astype(
        jnp.bfloat16
    )
    pick_item = (coords[1][:, None] == jnp.arange(item_tiles)[None, :]).astype(jnp.bfloat16)
    user_sel = jnp.einsum(
        "su,uiw->siw",
        pick_user,
        user_block.reshape(user_tiles, size, width),
        preferred_element_type=jnp.float32,
    ).astype(jnp.bfloat16)
    item_sel = jnp.einsum(
        "st,tjw->sjw",
        pick_item,
        item_block.reshape(item_tiles, size, width),
        preferred_element_type=jnp.float32,
    ).astype(jnp.bfloat16)
    to_users = jnp.einsum("sij,sjw->siw", tiles, item_sel, preferred_element_type=jnp.float32)
    to_items = jnp.einsum("sij,siw->sjw", tiles, user_sel, preferred_element_type=jnp.float32)
    part_users = jnp.einsum(
        "su,siw->uiw", pick_user.astype(jnp.float32), to_users, precision=lax.Precision.HIGHEST
    ).reshape(user_tiles * size, width)
    part_items = jnp.einsum(
        "st,sjw->tjw", pick_item.astype(jnp.float32), to_items, precision=lax.Precision.HIGHEST
    ).reshape(item_tiles * size, width)
    users_next = lax.psum_scatter(part_users, "col", scatter_dimension=0, tiled=True)
    items_next = lax.psum_scatter(part_items, "row", scatter_dimension=0, tiled=True)
    return (users_next.astype(jnp.bfloat16), items_next.astype(jnp.bfloat16))


def encode(values):
    rows, width = values.shape
    groups = values.reshape(rows // 8, 8, width)
    peak = jnp.maximum(jnp.max(jnp.abs(groups), axis=0), TINY)
    return encode_by(values, peak), peak


def encode_by(values, peak):
    rows, width = values.shape
    groups = values.reshape(rows // 8, 8, width)
    scaled = jnp.round(groups * (LEVELS / peak)[None])
    return scaled.astype(jnp.int32).astype(jnp.int16).reshape(rows, width)


def decode(code, peak):
    rows, width = code.shape
    groups = code.astype(jnp.int32).astype(jnp.float32).reshape(rows // 8, 8, width)
    return (groups * (peak * (1.0 / LEVELS))[None]).reshape(rows, width)


def kernel(
    n_z,
    coords_in,
    count_in,
    user_in,
    item_in,
    tile_in,
    out_u,
    out_i,
    u_all,
    i_got,
    r_own,
    r_near,
    s_sel,
    tile_v,
    tile_t,
    meta,
    metas,
    part_u,
    from_p,
    send_z,
    peak_z,
    from_z,
    from_zp,
    part_i,
    send_1,
    peak_1,
    from_1,
    from_1p,
    pair_1,
    pair_1p,
    fwd_1,
    mask_1p,
    fwd_1p,
    send_2,
    peak_2,
    from_2,
    from_2p,
    gauge,
    coords,
    load_sem,
    sent,
    first_s,
    late,
    uz_r,
    up_r,
    io_r,
    iq_r,
    ig_r,
    rp_r,
    rz_r,
    r1_r,
    rq_r,
    r2_r,
):
    row, col = lax.axis_index("row"), lax.axis_index("col")
    y, x = row // 2, row % 2
    z, core = col // 2, col % 2
    row_x, row_y = 2 * y + 1 - x, 2 * (1 - y) + x
    twin = 2 * z + 1 - core
    x_dev, y_dev, p_dev = (row_x, twin), (row_y, twin), (row, twin)
    high = z // (n_z // 2)

    def far_first(at):
        mirrored = z + high * (n_z - 1 - 2 * z)
        to = n_z - 1 - at
        to = jnp.where(to <= mirrored, to - 1, to)
        return to + high * (n_z - 1 - 2 * to)

    others = [far_first(at) for at in range(n_z - 1)]
    z_devs = [(row, 2 * at + 1 - core) for at in others]
    near_first = others[::-1]
    rows_u, rows_i = user_in.shape[0], i_got.shape[0] * i_got.shape[2]
    size = tile_v.shape[-1]
    width = user_in.shape[1]
    steps = send_1.shape[1]
    groups = peak_1.shape[0]
    half, each = rows_i // 2, steps // groups
    chunk = half // steps
    pieces = size // rows_u // 2
    sizes = []

    def user_slot(at):
        blocks = size // rows_u
        inner = pl.multiple_of(at % blocks * rows_u, rows_u)
        return u_all.at[at // blocks, pl.ds(inner, rows_u)]

    def rows_of(step):
        return pl.ds(step * chunk, chunk)

    def send(src, dst, recv, device):
        sizes.append(math.prod(src.shape) * src.dtype.itemsize)
        copy(src, dst, sent.at[0], recv, device).start()

    def copy(src, dst, sem, recv, device):
        return pltpu.make_async_remote_copy(
            src_ref=src,
            dst_ref=dst,
            send_sem=sem,
            recv_sem=recv,
            device_id=device,
            device_id_type=MESH,
        )

    def arrived(like, recv):
        copy(like, like, recv, recv, x_dev).wait_recv()

    def landed(recv, *likes):
        total = sum(math.prod(like.shape) * like.dtype.itemsize for like in likes)
        arrived(gauge.at[pl.ds(0, total // (4 * width))], recv)

    barrier = pltpu.get_barrier_semaphore()
    across, mates = z_devs[: n_z // 2], z_devs[n_z // 2 :]
    peers = [x_dev, y_dev, p_dev] + mates
    for peer in peers:
        pl.semaphore_signal(barrier, inc=1, device_id=peer, device_id_type=MESH)

    @pl.when(high == 0)
    def _():
        for peer in across:
            pl.semaphore_signal(barrier, inc=1, device_id=peer, device_id_type=MESH)

    loads = [
        pltpu.make_async_copy(user_in, user_slot(col), load_sem.at[0]),
        pltpu.make_async_copy(item_in, i_got.at[:, 0], load_sem.at[1]),
        pltpu.make_async_copy(tile_in, tile_v, load_sem.at[2]),
        pltpu.make_async_copy(coords_in, coords, load_sem.at[3]),
            ]
    for load in loads:
        load.start()

    loads[3].wait()
    tu, ti = coords[0], coords[1]
    meta[0] = jnp.full(meta.shape[1:], tu, jnp.int32)
    meta[1] = jnp.full(meta.shape[1:], ti, jnp.int32)
    my_tu, my_ti = meta[0][0:1, :], meta[1][0:1, :]
    live = jnp.full((1, width), count_in[0, 0], jnp.int32) > 0
    pl.semaphore_wait(barrier, len(peers) + high * len(across))

    loads[0].wait()
    own = user_slot(col)

    @pl.when(high == 1)
    def _():
        for peer in across:
            pl.semaphore_signal(late, inc=1, device_id=peer, device_id_type=MESH)
        copy(own, own, first_s.at[0], uz_r.at[z], across[0]).start()

    sizes.extend([rows_u * width * 2] * (len(across) - 1))
    for device in mates:
        send(own, own, uz_r.at[z], device)
    for at, device in enumerate((x_dev, y_dev, p_dev)):
        send(meta, metas.at[at], io_r.at[0], device)
    loads[1].wait()
    for step in range(steps):
        for part, device in ((0, x_dev), (1, y_dev)):
            send(
                i_got.at[part, 0, rows_of(step)],
                r_near.at[part, rows_of(step)],
                iq_r.at[step],
                device,
            )
    send(own, own, up_r.at[0], p_dev)
    for part in range(2):
        send(i_got.at[part, 0], r_own.at[part], io_r.at[0], p_dev)

    loads[2].wait()
    tile_t[...] = tile_v[...].reshape(size, size).T
    @pl.when(high == 1)
    def _():
        copy(own, own, first_s.at[0], uz_r.at[z], across[0]).wait_send()
        for device in across[1:]:
            copy(own, own, sent.at[0], uz_r.at[z], device).start()

    landed(io_r.at[0], metas, r_own)
    x_ti, y_ti, p_ti = (metas[at, 1][0:1, :] for at in range(3))
    p_tu = metas[2, 0][0:1, :]

    def pass_user(at):
        slot = user_slot(2 * at + 1 - core)
        arrived(slot, uz_r.at[at])
        copy(slot, slot, sent.at[0], up_r.at[0], p_dev).start()

    def pass_items(step):
        landed(iq_r.at[step], r_near.at[:, rows_of(step)])
        for part, want, near, device in ((0, y_ti, row_x, y_dev), (1, x_ti, row_y, x_dev)):
            here = (part, rows_of(step))
            s_sel[here] = jnp.where(want == near, r_near[here], r_own[here])
            copy(
                s_sel.at[here], i_got.at[part, 2, rows_of(step)], sent.at[0], ig_r.at[0], device
            ).start()
            copy(
                r_near.at[here], i_got.at[part, 1, rows_of(step)], sent.at[0], ig_r.at[0], p_dev
            ).start()

    users = [(pass_user, at) for at in near_first]
    items = [(pass_items, step) for step in range(steps)]
    sizes.extend([rows_u * width * 2] * len(users) + [chunk * width * 2] * (4 * steps))

    for step, at in users[: len(mates)]:
        step(at)

    @pl.when(high == 0)
    def _():
        pl.semaphore_wait(late, len(across))
        for device in across[:0:-1]:
            copy(own, own, sent.at[0], uz_r.at[z], device).start()
        copy(own, own, first_s.at[0], uz_r.at[z], across[0]).start()

    for step, at in items:
        step(at)

    def pass_across():
        for step, at in users[len(mates) :]:
            step(at)


    def users_product():
        arrived(i_got.at[:, pl.ds(1, 2)], ig_r.at[0])
        sel_x = jnp.where(ti == row, 0, jnp.where(ti == row_x, 1, 2))
        sel_y = jnp.where(ti == row, 0, jnp.where(ti == row_y, 1, 2))
        item_sel = jnp.concatenate([i_got[0, sel_x], i_got[1, sel_y]], axis=0)
        item_sel = jnp.where(live, item_sel, 0.0).astype(item_sel.dtype)

        def multiply(owner):
            rows = jnp.concatenate([tile_v[2 * h + owner] for h in range(pieces)], axis=0)
            product = jnp.dot(rows, item_sel, preferred_element_type=jnp.float32)
            for h in range(pieces):
                part_u[2 * h + owner] = product[h * rows_u : (h + 1) * rows_u]

        multiply(core)
        for h in range(pieces):
            copy(part_u.at[2 * h + core], from_p.at[h], sent.at[0], rp_r.at[0], p_dev).start()
        multiply(1 - core)

    def items_product():
        arrived(u_all.at[pl.ds(0, u_all.shape[0] // 2)], up_r.at[0])

        user_sel = u_all[tu]
        user_sel = jnp.where(live, user_sel, 0.0).astype(user_sel.dtype)
        for g in range(groups):
            rows = g * chunk * each
            lhs = [tile_t[part * half + rows : part * half + rows + chunk * each] for part in range(2)]
            product = jnp.dot(
                jnp.concatenate(lhs, axis=0), user_sel, preferred_element_type=jnp.float32
            )
            code, peak_1[g] = encode(product)
            some = slice(g * each, (g + 1) * each)
            send_1[:, some] = code.reshape(2, each, chunk, width)
            for part, device in enumerate((x_dev, y_dev)):
                copy(
                    peak_1.at[g], from_1p.at[part, g], sent.at[0], r1_r.at[g * each], device
                ).start()
            for step in range(g * each, (g + 1) * each):
                for part, device in enumerate((x_dev, y_dev)):
                    here = (part, step)
                    copy(
                        send_1.at[here], from_1.at[here], sent.at[0], r1_r.at[step], device
                    ).start()
            part_i[:, some] = product.reshape(2, each, chunk, width)
        copy(peak_1, pair_1p, sent.at[0], rq_r.at[0], p_dev).start()
        copy(send_1, pair_1, sent.at[0], rq_r.at[0], p_dev).start()

    for ref in (from_p, peak_1, peak_1, peak_1, send_1, send_1):
        sizes.append(math.prod(ref.shape) * ref.dtype.itemsize)

    def users_out():
        arrived(from_p, rp_r.at[0])
        to = list(zip(others, z_devs))
        for at, device in to[:1] + to[n_z // 2 :] + [(z, p_dev)] + to[1 : n_z // 2]:
            tile, h = at // pieces, at % pieces
            send_z[at], peak_z[at] = encode(
                jnp.where(my_tu == tile, part_u[2 * h + 1 - core], 0.0)
                + jnp.where(p_tu == tile, from_p[h], 0.0)
            )
            copy(peak_z.at[at], from_zp.at[z], sent.at[0], rz_r.at[0], device).start()
            copy(send_z.at[at], from_z.at[z], sent.at[0], rz_r.at[0], device).start()

    def items_out():
        landed(rq_r.at[0], pair_1, pair_1p)
        sides = ((0, x_ti, row_y, y_dev), (1, y_ti, row_x, x_dev))
        for step in range(steps):
            g = step // each
            if step % each == 0:
                landed(r1_r.at[step], from_1.at[:, step], from_1p.at[:, g])
                for part, other, owner, device in sides:
                    mask_1p[part, g] = jnp.where(other == row, from_1p[part, g], 0.0)
                    peak_2[part, g] = jnp.where(p_ti == owner, pair_1p[g], 0.0) + jnp.where(
                        other == owner, from_1p[part, g], TINY
                    )
                    copy(
                        peak_2.at[part, g], from_2p.at[part, g], sent.at[0], r2_r.at[step], device
                    ).start()
            else:
                landed(r1_r.at[step], from_1.at[:, step])
            for part, other, owner, device in sides:
                here = (part, step)
                send_2[here] = encode_by(
                    jnp.where(p_ti == owner, decode(pair_1[here], pair_1p[g]), 0.0)
                    + jnp.where(other == owner, decode(from_1[here], from_1p[part, g]), 0.0),
                    peak_2[part, g],
                )
                copy(
                    send_2.at[here], from_2.at[here], sent.at[0], r2_r.at[step], device
                ).start()
            for part in range(2):
                here = (part, step)
                copy(from_1.at[here], fwd_1.at[here], sent.at[0], r2_r.at[0], p_dev).start()
        copy(mask_1p, fwd_1p, sent.at[0], r2_r.at[0], p_dev).start()

    for ref in (peak_z, send_z, mask_1p, peak_2, send_2, from_1):
        sizes.append(math.prod(ref.shape) * ref.dtype.itemsize)

    @pl.when(high == 0)
    def _():
        pass_across()
        items_product()
        users_product()
        users_out()
        items_out()

    @pl.when(high == 1)
    def _():
        pass_across()
        users_product()
        items_product()
        users_out()
        items_out()


    for step in range(steps):
        g = step // each
        if step == 0:
            landed(r2_r.at[0], from_2.at[:, 0], from_2p.at[:, 0], fwd_1, fwd_1p)
        elif step % each == 0:
            landed(r2_r.at[step], from_2.at[:, step], from_2p.at[:, g])
        else:
            landed(r2_r.at[step], from_2.at[:, step])
        for part in range(2):
            here = (part, step)
            last = jnp.where(my_ti == row, part_i[here], 0.0)
            last = last + decode(fwd_1[here], fwd_1p[part, g])
            last = last + decode(from_2[here], from_2p[part, g])
            start = part * half + step * chunk
            out_i[pl.ds(start, chunk), :] = last.astype(out_i.dtype)

    landed(rz_r.at[0], from_z, from_zp)
    total = decode(from_z[0], from_zp[0])
    for at in range(1, n_z):
        total = total + decode(from_z[at], from_zp[at])
    out_u[...] = total.astype(out_u.dtype)

    @pl.when(high == 0)
    def _():
        copy(own, own, first_s.at[0], uz_r.at[z], across[0]).wait_send()

    like = gauge.at[pl.ds(0, sum(sizes) // (4 * width))]
    copy(like, like, sent.at[0], sent.at[0], x_dev).wait_send()


def put(users, items, out_u, out_i, sems):
    copies = [
        pltpu.make_async_copy(users, out_u, sems.at[0]),
        pltpu.make_async_copy(items, out_i, sems.at[1]),
    ]
    for c in copies:
        c.start()
    for c in copies:
        c.wait()


def planned(user_feats, item_feats, tile_values, tile_coords, tile_count, *, n_z):
    rows_u, width = user_feats.shape
    rows_i = item_feats.shape[0]
    size = tile_values.shape[-1]
    f32, bf16, dma = jnp.float32, jnp.bfloat16, pltpu.SemaphoreType.DMA
    blocks = size // rows_u
    vmem = pl.BlockSpec(memory_space=pltpu.VMEM)
    anywhere = pl.BlockSpec(memory_space=pl.ANY)
    cut = (2, STEPS, rows_i // (2 * STEPS), width)
    peak = (8, width)
    i16 = jnp.int16
    vm = pltpu.VMEM
    outs = pl.pallas_call(
        functools.partial(kernel, n_z),
        out_shape=(pltpu.VMEM((rows_u, width), bf16), pltpu.VMEM((rows_i, width), bf16)),
        in_specs=[anywhere, pl.BlockSpec(memory_space=pltpu.SMEM)] + [anywhere] * 3,
        out_specs=(vmem, vmem),
        scratch_shapes=[
            vm((2 * n_z * rows_u // size, size, width), bf16),
            vm((2, 3, rows_i // 2, width), bf16),
            vm((2, rows_i // 2, width), bf16),
            vm((2, rows_i // 2, width), bf16),
            vm((2, rows_i // 2, width), bf16),
            vm((blocks, rows_u, size), bf16),
            vm((size, size), bf16),
            vm((2,) + peak, jnp.int32),
            vm((3, 2) + peak, jnp.int32),
            vm((blocks, rows_u, width), f32),
            vm((blocks // 2, rows_u, width), f32),
            vm((n_z, rows_u, width), i16),
            vm((n_z,) + peak, f32),
            vm((n_z, rows_u, width), i16),
            vm((n_z,) + peak, f32),
            vm(cut, f32),
            vm(cut, i16),
            vm((GROUPS,) + peak, f32),
            vm(cut, i16),
            vm((2, GROUPS) + peak, f32),
            vm(cut, i16),
            vm((GROUPS,) + peak, f32),
            vm(cut, i16),
            vm((2, GROUPS) + peak, f32),
            vm((2, GROUPS) + peak, f32),
            vm(cut, i16),
            vm((2, GROUPS) + peak, f32),
            vm(cut, i16),
            vm((2, GROUPS) + peak, f32),
            vm((16 * rows_i, width), f32),
            pltpu.SMEM((2,), jnp.int32),
        ]
        + [dma((n,)) for n in (4, 1, 1)]
        + [pltpu.SemaphoreType.REGULAR]
        + [dma((n,)) for n in (n_z, 1, 1, STEPS, 1, 1, 1, STEPS, 1, STEPS)],
        compiler_params=pltpu.CompilerParams(collective_id=0, has_side_effects=True),
    )(
        tile_coords.reshape(2),
        tile_count,
        user_feats,
        item_feats.reshape(2, rows_i // 2, width),
        tile_values.reshape(blocks, rows_u, size),
    )
    return pl.pallas_call(
        put,
        out_shape=[jax.ShapeDtypeStruct(out.shape, out.dtype) for out in outs],
        in_specs=[vmem, vmem],
        out_specs=[anywhere, anywhere],
        scratch_shapes=[dma((2,))],
    )(*[pltpu.with_memory_space_constraint(out, pltpu.VMEM) for out in outs])


def solution(mesh):
    n_row, n_col = mesh.shape["row"], mesh.shape["col"]

    def local(user_feats, item_feats, tile_values, tile_coords, tile_count):
        slots, size = tile_values.shape[2], tile_values.shape[3]
        rows_u = user_feats.shape[0]
        fits = (
            n_row == 4
            and n_col % 2 == 0
            and slots == 1
            and item_feats.shape[0] == size
            and size % (2 * rows_u) == 0
            and size % (32 * STEPS) == 0
            and n_col * rows_u % (2 * size) == 0
            and (n_col // 2 - 1) * rows_u <= size
        )
        args = (user_feats, item_feats, tile_values, tile_coords, tile_count)
        return planned(*args, n_z=n_col // 2) if fits else gathered(*args)

    placed = (
        P(("row", "col"), None),
        P(("col", "row"), None),
        P("row", "col", None, None, None),
        P("row", "col", None, None),
        P("row", "col"),
    )
    return jax.shard_map(
        local,
        mesh=mesh,
        in_specs=placed,
        out_specs=(P(("row", "col"), None), P(("col", "row"), None)),
        check_vma=False,
    )
```

```python
import functools
import math

import jax
import jax.numpy as jnp
from jax import lax
from jax.experimental import pallas as pl
from jax.experimental.pallas import tpu as pltpu
from jax.sharding import PartitionSpec as P

MESH = pl.DeviceIdType.MESH
LEVELS = 32760.0
STEPS = 4
GROUPS = 2
TINY = 1e-30


def gathered(user_feats, item_feats, tile_values, tile_coords, tile_count):
    user_block = lax.all_gather(user_feats, "col", axis=0, tiled=True)
    item_block = lax.all_gather(item_feats, "row", axis=0, tiled=True)
    tiles = tile_values[0, 0]
    coords = tile_coords[0, 0]
    count = tile_count[0, 0]
    slots = tiles.shape[0]
    size = tiles.shape[1]
    width = user_block.shape[1]
    user_tiles = user_block.shape[0] // size
    item_tiles = item_block.shape[0] // size
    live = jnp.arange(slots) < count
    pick_user = ((coords[0][:, None] == jnp.arange(user_tiles)[None, :]) & live[:, None]).astype(
        jnp.bfloat16
    )
    pick_item = (coords[1][:, None] == jnp.arange(item_tiles)[None, :]).astype(jnp.bfloat16)
    user_sel = jnp.einsum(
        "su,uiw->siw",
        pick_user,
        user_block.reshape(user_tiles, size, width),
        preferred_element_type=jnp.float32,
    ).astype(jnp.bfloat16)
    item_sel = jnp.einsum(
        "st,tjw->sjw",
        pick_item,
        item_block.reshape(item_tiles, size, width),
        preferred_element_type=jnp.float32,
    ).astype(jnp.bfloat16)
    to_users = jnp.einsum("sij,sjw->siw", tiles, item_sel, preferred_element_type=jnp.float32)
    to_items = jnp.einsum("sij,siw->sjw", tiles, user_sel, preferred_element_type=jnp.float32)
    part_users = jnp.einsum(
        "su,siw->uiw", pick_user.astype(jnp.float32), to_users, precision=lax.Precision.HIGHEST
    ).reshape(user_tiles * size, width)
    part_items = jnp.einsum(
        "st,sjw->tjw", pick_item.astype(jnp.float32), to_items, precision=lax.Precision.HIGHEST
    ).reshape(item_tiles * size, width)
    users_next = lax.psum_scatter(part_users, "col", scatter_dimension=0, tiled=True)
    items_next = lax.psum_scatter(part_items, "row", scatter_dimension=0, tiled=True)
    return (users_next.astype(jnp.bfloat16), items_next.astype(jnp.bfloat16))


def encode(values):
    rows, width = values.shape
    groups = values.reshape(rows // 8, 8, width)
    peak = jnp.maximum(jnp.max(jnp.abs(groups), axis=0), TINY)
    return encode_by(values, peak), peak


def encode_by(values, peak):
    rows, width = values.shape
    groups = values.reshape(rows // 8, 8, width)
    scaled = jnp.round(groups * (LEVELS / peak)[None])
    return scaled.astype(jnp.int32).astype(jnp.int16).reshape(rows, width)


def decode(code, peak):
    rows, width = code.shape
    groups = code.astype(jnp.int32).astype(jnp.float32).reshape(rows // 8, 8, width)
    return (groups * (peak * (1.0 / LEVELS))[None]).reshape(rows, width)


def kernel(
    n_z,
    coords_in,
    count_in,
    user_in,
    item_in,
    tile_in,
    out_u,
    out_i,
    u_all,
    i_got,
    r_own,
    r_near,
    s_sel,
    tile_v,
    tile_t,
    meta,
    metas,
    part_u,
    from_p,
    send_z,
    peak_z,
    from_z,
    from_zp,
    part_i,
    send_1,
    peak_1,
    from_1,
    from_1p,
    pair_1,
    pair_1p,
    fwd_1,
    mask_1p,
    fwd_1p,
    send_2,
    peak_2,
    from_2,
    from_2p,
    gauge,
    coords,
    load_sem,
    sent,
    first_s,
    late,
    uz_r,
    up_r,
    io_r,
    iq_r,
    ig_r,
    rp_r,
    rz_r,
    r1_r,
    rq_r,
    r2_r,
):
    row, col = lax.axis_index("row"), lax.axis_index("col")
    y, x = row // 2, row % 2
    z, core = col // 2, col % 2
    row_x, row_y = 2 * y + 1 - x, 2 * (1 - y) + x
    twin = 2 * z + 1 - core
    x_dev, y_dev, p_dev = (row_x, twin), (row_y, twin), (row, twin)
    high = z // (n_z // 2)

    def far_first(at):
        mirrored = z + high * (n_z - 1 - 2 * z)
        to = n_z - 1 - at
        to = jnp.where(to <= mirrored, to - 1, to)
        return to + high * (n_z - 1 - 2 * to)

    others = [far_first(at) for at in range(n_z - 1)]
    z_devs = [(row, 2 * at + 1 - core) for at in others]
    near_first = others[::-1]
    rows_u, rows_i = user_in.shape[0], i_got.shape[0] * i_got.shape[2]
    size = tile_v.shape[-1]
    width = user_in.shape[1]
    steps = send_1.shape[1]
    groups = peak_1.shape[0]
    half, each = rows_i // 2, steps // groups
    chunk = half // steps
    pieces = size // rows_u // 2
    turns = [(others[0] + step) % pieces for step in range(pieces)]
    sizes = []

    def user_slot(at):
        blocks = size // rows_u
        inner = pl.multiple_of(at % blocks * rows_u, rows_u)
        return u_all.at[at // blocks, pl.ds(inner, rows_u)]

    def rows_of(step):
        return pl.ds(step * chunk, chunk)

    def send(src, dst, recv, device):
        sizes.append(math.prod(src.shape) * src.dtype.itemsize)
        copy(src, dst, sent.at[0], recv, device).start()

    def copy(src, dst, sem, recv, device):
        return pltpu.make_async_remote_copy(
            src_ref=src,
            dst_ref=dst,
            send_sem=sem,
            recv_sem=recv,
            device_id=device,
            device_id_type=MESH,
        )

    def arrived(like, recv):
        copy(like, like, recv, recv, x_dev).wait_recv()

    def landed(recv, *likes):
        total = sum(math.prod(like.shape) * like.dtype.itemsize for like in likes)
        arrived(gauge.at[pl.ds(0, total // (4 * width))], recv)

    barrier = pltpu.get_barrier_semaphore()
    across, mates = z_devs[: n_z // 2], z_devs[n_z // 2 :]
    peers = [x_dev, y_dev, p_dev] + mates
    for peer in peers:
        pl.semaphore_signal(barrier, inc=1, device_id=peer, device_id_type=MESH)

    @pl.when(high == 0)
    def _():
        for peer in across:
            pl.semaphore_signal(barrier, inc=1, device_id=peer, device_id_type=MESH)

    loads = [
        pltpu.make_async_copy(user_in, user_slot(col), load_sem.at[0]),
        pltpu.make_async_copy(item_in, i_got.at[:, 0], load_sem.at[1]),
        pltpu.make_async_copy(tile_in, tile_v, load_sem.at[2]),
        pltpu.make_async_copy(coords_in, coords, load_sem.at[3]),
            ]
    for load in loads:
        load.start()

    loads[3].wait()
    tu, ti = coords[0], coords[1]
    meta[0] = jnp.full(meta.shape[1:], tu, jnp.int32)
    meta[1] = jnp.full(meta.shape[1:], ti, jnp.int32)
    my_tu, my_ti = meta[0][0:1, :], meta[1][0:1, :]
    live = jnp.full((1, width), count_in[0, 0], jnp.int32) > 0
    pl.semaphore_wait(barrier, len(peers) + high * len(across))

    loads[0].wait()
    own = user_slot(col)

    @pl.when(high == 1)
    def _():
        for peer in across:
            pl.semaphore_signal(late, inc=1, device_id=peer, device_id_type=MESH)
        copy(own, own, first_s.at[0], uz_r.at[z], across[0]).start()

    sizes.extend([rows_u * width * 2] * (len(across) - 1))
    for device in mates:
        send(own, own, uz_r.at[z], device)
    for at, device in enumerate((x_dev, y_dev, p_dev)):
        send(meta, metas.at[at], io_r.at[0], device)
    loads[1].wait()
    for step in range(steps):
        for part, device in ((0, x_dev), (1, y_dev)):
            send(
                i_got.at[part, 0, rows_of(step)],
                r_near.at[part, rows_of(step)],
                iq_r.at[step],
                device,
            )
    send(own, own, up_r.at[0], p_dev)
    for part in range(2):
        send(i_got.at[part, 0], r_own.at[part], io_r.at[0], p_dev)

    loads[2].wait()
    tile_t[...] = tile_v[...].reshape(size, size).T
    @pl.when(high == 1)
    def _():
        copy(own, own, first_s.at[0], uz_r.at[z], across[0]).wait_send()
        for device in across[1:]:
            copy(own, own, sent.at[0], uz_r.at[z], device).start()

    landed(io_r.at[0], metas, r_own)
    x_ti, y_ti, p_ti = (metas[at, 1][0:1, :] for at in range(3))
    p_tu = metas[2, 0][0:1, :]

    def pass_user(at):
        slot = user_slot(2 * at + 1 - core)
        arrived(slot, uz_r.at[at])
        copy(slot, slot, sent.at[0], up_r.at[0], p_dev).start()

    def pass_items(step):
        landed(iq_r.at[step], r_near.at[:, rows_of(step)])
        for part, want, near, device in ((0, y_ti, row_x, y_dev), (1, x_ti, row_y, x_dev)):
            here = (part, rows_of(step))
            s_sel[here] = jnp.where(want == near, r_near[here], r_own[here])
            copy(
                s_sel.at[here], i_got.at[part, 2, rows_of(step)], sent.at[0], ig_r.at[0], device
            ).start()
            copy(
                r_near.at[here], i_got.at[part, 1, rows_of(step)], sent.at[0], ig_r.at[0], p_dev
            ).start()

    users = [(pass_user, at) for at in near_first]
    items = [(pass_items, step) for step in range(steps)]
    sizes.extend([rows_u * width * 2] * len(users) + [chunk * width * 2] * (4 * steps))

    for step, at in users[: len(mates)]:
        step(at)

    @pl.when(high == 0)
    def _():
        pl.semaphore_wait(late, len(across))
        for device in across[:0:-1]:
            copy(own, own, sent.at[0], uz_r.at[z], device).start()
        copy(own, own, first_s.at[0], uz_r.at[z], across[0]).start()

    for step, at in items:
        step(at)

    def pass_across():
        for step, at in users[len(mates) :]:
            step(at)


    def users_product():
        arrived(i_got.at[:, pl.ds(1, 2)], ig_r.at[0])
        sel_x = jnp.where(ti == row, 0, jnp.where(ti == row_x, 1, 2))
        sel_y = jnp.where(ti == row, 0, jnp.where(ti == row_y, 1, 2))
        item_sel = jnp.concatenate([i_got[0, sel_x], i_got[1, sel_y]], axis=0)
        item_sel = jnp.where(live, item_sel, 0.0).astype(item_sel.dtype)

        def multiply(some):
            rows = jnp.concatenate([tile_v[b] for b in some], axis=0)
            product = jnp.dot(rows, item_sel, preferred_element_type=jnp.float32)
            for at, b in enumerate(some):
                part_u[b] = product[at * rows_u : (at + 1) * rows_u]

        multiply([2 * h + core for h in turns])
        for h in turns:
            copy(part_u.at[2 * h + core], from_p.at[h], sent.at[0], rp_r.at[h], p_dev).start()
        multiply([2 * h + 1 - core for h in range(pieces)])

    def items_product():
        arrived(u_all.at[pl.ds(0, u_all.shape[0] // 2)], up_r.at[0])

        user_sel = u_all[tu]
        user_sel = jnp.where(live, user_sel, 0.0).astype(user_sel.dtype)
        for g in range(groups):
            rows = g * chunk * each
            lhs = [tile_t[part * half + rows : part * half + rows + chunk * each] for part in range(2)]
            product = jnp.dot(
                jnp.concatenate(lhs, axis=0), user_sel, preferred_element_type=jnp.float32
            )
            code, peak_1[g] = encode(product)
            some = slice(g * each, (g + 1) * each)
            send_1[:, some] = code.reshape(2, each, chunk, width)
            for part, device in enumerate((x_dev, y_dev)):
                copy(
                    peak_1.at[g], from_1p.at[part, g], sent.at[0], r1_r.at[g * each], device
                ).start()
            for step in range(g * each, (g + 1) * each):
                for part, device in enumerate((x_dev, y_dev)):
                    here = (part, step)
                    copy(
                        send_1.at[here], from_1.at[here], sent.at[0], r1_r.at[step], device
                    ).start()
            part_i[:, some] = product.reshape(2, each, chunk, width)
        copy(peak_1, pair_1p, sent.at[0], rq_r.at[0], p_dev).start()
        copy(send_1, pair_1, sent.at[0], rq_r.at[0], p_dev).start()

    for ref in (from_p, peak_1, peak_1, peak_1, send_1, send_1):
        sizes.append(math.prod(ref.shape) * ref.dtype.itemsize)

    targets = list(zip(others, z_devs))
    targets = targets[:1] + targets[n_z // 2 :] + [(z, p_dev)] + targets[1 : n_z // 2]

    def users_out(ready, some):
        for h in ready:
            arrived(from_p.at[h], rp_r.at[h])
        for at, device in some:
            tile, h = at // pieces, at % pieces
            send_z[at], peak_z[at] = encode(
                jnp.where(my_tu == tile, part_u[2 * h + 1 - core], 0.0)
                + jnp.where(p_tu == tile, from_p[h], 0.0)
            )
            copy(peak_z.at[at], from_zp.at[z], sent.at[0], rz_r.at[0], device).start()
            copy(send_z.at[at], from_z.at[z], sent.at[0], rz_r.at[0], device).start()

    def users_first():
        users_out(turns[:1], targets[:1])

    def users_rest():
        users_out(turns[1:], targets[1:])

    def items_out():
        landed(rq_r.at[0], pair_1, pair_1p)
        sides = ((0, x_ti, row_y, y_dev), (1, y_ti, row_x, x_dev))
        for step in range(steps):
            g = step // each
            if step % each == 0:
                landed(r1_r.at[step], from_1.at[:, step], from_1p.at[:, g])
                for part, other, owner, device in sides:
                    mask_1p[part, g] = jnp.where(other == row, from_1p[part, g], 0.0)
                    peak_2[part, g] = jnp.where(p_ti == owner, pair_1p[g], 0.0) + jnp.where(
                        other == owner, from_1p[part, g], TINY
                    )
                    copy(
                        peak_2.at[part, g], from_2p.at[part, g], sent.at[0], r2_r.at[step], device
                    ).start()
            else:
                landed(r1_r.at[step], from_1.at[:, step])
            for part, other, owner, device in sides:
                here = (part, step)
                send_2[here] = encode_by(
                    jnp.where(p_ti == owner, decode(pair_1[here], pair_1p[g]), 0.0)
                    + jnp.where(other == owner, decode(from_1[here], from_1p[part, g]), 0.0),
                    peak_2[part, g],
                )
                copy(
                    send_2.at[here], from_2.at[here], sent.at[0], r2_r.at[step], device
                ).start()
            for part in range(2):
                here = (part, step)
                copy(from_1.at[here], fwd_1.at[here], sent.at[0], r2_r.at[0], p_dev).start()
        copy(mask_1p, fwd_1p, sent.at[0], r2_r.at[0], p_dev).start()

    for ref in (peak_z, send_z, mask_1p, peak_2, send_2, from_1):
        sizes.append(math.prod(ref.shape) * ref.dtype.itemsize)

    def run(*stages):
        for stage in stages:
            stage()

    @pl.when(high == 0)
    def _():
        run(pass_across, items_product, users_product, users_first, users_rest, items_out)

    @pl.when(jnp.logical_and(high == 1, z < n_z - 1))
    def _():
        run(pass_across, users_product, items_product, users_first, users_rest, items_out)

    @pl.when(z == n_z - 1)
    def _():
        run(pass_across, users_product, users_first, items_product, users_rest, items_out)

    for step in range(steps):
        g = step // each
        if step == 0:
            landed(r2_r.at[0], from_2.at[:, 0], from_2p.at[:, 0], fwd_1, fwd_1p)
        elif step % each == 0:
            landed(r2_r.at[step], from_2.at[:, step], from_2p.at[:, g])
        else:
            landed(r2_r.at[step], from_2.at[:, step])
        for part in range(2):
            here = (part, step)
            last = jnp.where(my_ti == row, part_i[here], 0.0)
            last = last + decode(fwd_1[here], fwd_1p[part, g])
            last = last + decode(from_2[here], from_2p[part, g])
            start = part * half + step * chunk
            out_i[pl.ds(start, chunk), :] = last.astype(out_i.dtype)

    landed(rz_r.at[0], from_z, from_zp)
    total = decode(from_z[0], from_zp[0])
    for at in range(1, n_z):
        total = total + decode(from_z[at], from_zp[at])
    out_u[...] = total.astype(out_u.dtype)

    @pl.when(high == 0)
    def _():
        copy(own, own, first_s.at[0], uz_r.at[z], across[0]).wait_send()

    like = gauge.at[pl.ds(0, sum(sizes) // (4 * width))]
    copy(like, like, sent.at[0], sent.at[0], x_dev).wait_send()


def put(users, items, out_u, out_i, sems):
    copies = [
        pltpu.make_async_copy(users, out_u, sems.at[0]),
        pltpu.make_async_copy(items, out_i, sems.at[1]),
    ]
    for c in copies:
        c.start()
    for c in copies:
        c.wait()


def planned(user_feats, item_feats, tile_values, tile_coords, tile_count, *, n_z):
    rows_u, width = user_feats.shape
    rows_i = item_feats.shape[0]
    size = tile_values.shape[-1]
    f32, bf16, dma = jnp.float32, jnp.bfloat16, pltpu.SemaphoreType.DMA
    blocks = size // rows_u
    vmem = pl.BlockSpec(memory_space=pltpu.VMEM)
    anywhere = pl.BlockSpec(memory_space=pl.ANY)
    cut = (2, STEPS, rows_i // (2 * STEPS), width)
    peak = (8, width)
    i16 = jnp.int16
    vm = pltpu.VMEM
    outs = pl.pallas_call(
        functools.partial(kernel, n_z),
        out_shape=(pltpu.VMEM((rows_u, width), bf16), pltpu.VMEM((rows_i, width), bf16)),
        in_specs=[anywhere, pl.BlockSpec(memory_space=pltpu.SMEM)] + [anywhere] * 3,
        out_specs=(vmem, vmem),
        scratch_shapes=[
            vm((2 * n_z * rows_u // size, size, width), bf16),
            vm((2, 3, rows_i // 2, width), bf16),
            vm((2, rows_i // 2, width), bf16),
            vm((2, rows_i // 2, width), bf16),
            vm((2, rows_i // 2, width), bf16),
            vm((blocks, rows_u, size), bf16),
            vm((size, size), bf16),
            vm((2,) + peak, jnp.int32),
            vm((3, 2) + peak, jnp.int32),
            vm((blocks, rows_u, width), f32),
            vm((blocks // 2, rows_u, width), f32),
            vm((n_z, rows_u, width), i16),
            vm((n_z,) + peak, f32),
            vm((n_z, rows_u, width), i16),
            vm((n_z,) + peak, f32),
            vm(cut, f32),
            vm(cut, i16),
            vm((GROUPS,) + peak, f32),
            vm(cut, i16),
            vm((2, GROUPS) + peak, f32),
            vm(cut, i16),
            vm((GROUPS,) + peak, f32),
            vm(cut, i16),
            vm((2, GROUPS) + peak, f32),
            vm((2, GROUPS) + peak, f32),
            vm(cut, i16),
            vm((2, GROUPS) + peak, f32),
            vm(cut, i16),
            vm((2, GROUPS) + peak, f32),
            vm((16 * rows_i, width), f32),
            pltpu.SMEM((2,), jnp.int32),
        ]
        + [dma((n,)) for n in (4, 1, 1)]
        + [pltpu.SemaphoreType.REGULAR]
        + [dma((n,)) for n in (n_z, 1, 1, STEPS, 1, blocks // 2, 1, STEPS, 1, STEPS)],
        compiler_params=pltpu.CompilerParams(collective_id=0, has_side_effects=True),
    )(
        tile_coords.reshape(2),
        tile_count,
        user_feats,
        item_feats.reshape(2, rows_i // 2, width),
        tile_values.reshape(blocks, rows_u, size),
    )
    return pl.pallas_call(
        put,
        out_shape=[jax.ShapeDtypeStruct(out.shape, out.dtype) for out in outs],
        in_specs=[vmem, vmem],
        out_specs=[anywhere, anywhere],
        scratch_shapes=[dma((2,))],
    )(*[pltpu.with_memory_space_constraint(out, pltpu.VMEM) for out in outs])


def solution(mesh):
    n_row, n_col = mesh.shape["row"], mesh.shape["col"]

    def local(user_feats, item_feats, tile_values, tile_coords, tile_count):
        slots, size = tile_values.shape[2], tile_values.shape[3]
        rows_u = user_feats.shape[0]
        fits = (
            n_row == 4
            and n_col % 2 == 0
            and slots == 1
            and item_feats.shape[0] == size
            and size % (2 * rows_u) == 0
            and size % (32 * STEPS) == 0
            and n_col * rows_u % (2 * size) == 0
            and (n_col // 2 - 1) * rows_u <= size
        )
        args = (user_feats, item_feats, tile_values, tile_coords, tile_count)
        return planned(*args, n_z=n_col // 2) if fits else gathered(*args)

    placed = (
        P(("row", "col"), None),
        P(("col", "row"), None),
        P("row", "col", None, None, None),
        P("row", "col", None, None),
        P("row", "col"),
    )
    return jax.shard_map(
        local,
        mesh=mesh,
        in_specs=placed,
        out_specs=(P(("row", "col"), None), P(("col", "row"), None)),
        check_vma=False,
    )
```

```python
import functools
import math

import jax
import jax.numpy as jnp
from jax import lax
from jax.experimental import pallas as pl
from jax.experimental.pallas import tpu as pltpu
from jax.sharding import PartitionSpec as P

MESH = pl.DeviceIdType.MESH
LEVELS = 32760.0
STEPS = 8
GROUPS = 2
TINY = 1e-30


def gathered(user_feats, item_feats, tile_values, tile_coords, tile_count):
    user_block = lax.all_gather(user_feats, "col", axis=0, tiled=True)
    item_block = lax.all_gather(item_feats, "row", axis=0, tiled=True)
    tiles = tile_values[0, 0]
    coords = tile_coords[0, 0]
    count = tile_count[0, 0]
    slots = tiles.shape[0]
    size = tiles.shape[1]
    width = user_block.shape[1]
    user_tiles = user_block.shape[0] // size
    item_tiles = item_block.shape[0] // size
    live = jnp.arange(slots) < count
    pick_user = ((coords[0][:, None] == jnp.arange(user_tiles)[None, :]) & live[:, None]).astype(
        jnp.bfloat16
    )
    pick_item = (coords[1][:, None] == jnp.arange(item_tiles)[None, :]).astype(jnp.bfloat16)
    user_sel = jnp.einsum(
        "su,uiw->siw",
        pick_user,
        user_block.reshape(user_tiles, size, width),
        preferred_element_type=jnp.float32,
    ).astype(jnp.bfloat16)
    item_sel = jnp.einsum(
        "st,tjw->sjw",
        pick_item,
        item_block.reshape(item_tiles, size, width),
        preferred_element_type=jnp.float32,
    ).astype(jnp.bfloat16)
    to_users = jnp.einsum("sij,sjw->siw", tiles, item_sel, preferred_element_type=jnp.float32)
    to_items = jnp.einsum("sij,siw->sjw", tiles, user_sel, preferred_element_type=jnp.float32)
    part_users = jnp.einsum(
        "su,siw->uiw", pick_user.astype(jnp.float32), to_users, precision=lax.Precision.HIGHEST
    ).reshape(user_tiles * size, width)
    part_items = jnp.einsum(
        "st,sjw->tjw", pick_item.astype(jnp.float32), to_items, precision=lax.Precision.HIGHEST
    ).reshape(item_tiles * size, width)
    users_next = lax.psum_scatter(part_users, "col", scatter_dimension=0, tiled=True)
    items_next = lax.psum_scatter(part_items, "row", scatter_dimension=0, tiled=True)
    return (users_next.astype(jnp.bfloat16), items_next.astype(jnp.bfloat16))


def encode(values):
    rows, width = values.shape
    groups = values.reshape(rows // 8, 8, width)
    peak = jnp.max(jnp.max(jnp.abs(groups), axis=0), axis=0, keepdims=True)
    peak = jnp.maximum(peak, TINY)
    return encode_by(values, peak), peak


def encode_by(values, peak):
    rows, width = values.shape
    groups = values.reshape(rows // 8, 8, width)
    scaled = jnp.round(groups * (LEVELS / peak)[None])
    return scaled.astype(jnp.int32).astype(jnp.int16).reshape(rows, width)


def decode(code, peak):
    rows, width = code.shape
    groups = code.astype(jnp.int32).astype(jnp.float32).reshape(rows // 8, 8, width)
    return (groups * (peak * (1.0 / LEVELS))[None]).reshape(rows, width)


def kernel(
    n_z,
    coords_in,
    count_in,
    user_in,
    item_in,
    tile_in,
    out_u,
    out_i,
    u_all,
    i_got,
    r_own,
    r_near,
    s_sel,
    tile_v,
    tile_t,
    meta,
    metas,
    part_u,
    from_p,
    send_z,
    peak_z,
    from_z,
    from_zp,
    part_i,
    send_1,
    peak_1,
    from_1,
    from_1p,
    pair_1,
    pair_1p,
    fwd_1,
    mask_1p,
    fwd_1p,
    send_2,
    peak_2,
    from_2,
    from_2p,
    gauge,
    coords,
    load_sem,
    sent,
    first_s,
    late,
    uz_r,
    up_r,
    io_r,
    iq_r,
    ig_r,
    rp_r,
    rz_r,
    r1_r,
    rq_r,
    r2_r,
):
    row, col = lax.axis_index("row"), lax.axis_index("col")
    y, x = row // 2, row % 2
    z, core = col // 2, col % 2
    row_x, row_y = 2 * y + 1 - x, 2 * (1 - y) + x
    twin = 2 * z + 1 - core
    x_dev, y_dev, p_dev = (row_x, twin), (row_y, twin), (row, twin)
    high = z // (n_z // 2)

    def far_first(at):
        mirrored = z + high * (n_z - 1 - 2 * z)
        to = n_z - 1 - at
        to = jnp.where(to <= mirrored, to - 1, to)
        return to + high * (n_z - 1 - 2 * to)

    others = [far_first(at) for at in range(n_z - 1)]
    z_devs = [(row, 2 * at + 1 - core) for at in others]
    near_first = others[::-1]
    rows_u, rows_i = user_in.shape[0], i_got.shape[0] * i_got.shape[2]
    size = tile_v.shape[-1]
    width = user_in.shape[1]
    steps = send_1.shape[1]
    groups = peak_1.shape[0]
    half, each = rows_i // 2, steps // groups
    chunk = half // steps
    pieces = size // rows_u // 2
    turns = [(others[0] + step) % pieces for step in range(pieces)]
    sizes = []

    def user_slot(at):
        blocks = size // rows_u
        inner = pl.multiple_of(at % blocks * rows_u, rows_u)
        return u_all.at[at // blocks, pl.ds(inner, rows_u)]

    def rows_of(step):
        return pl.ds(step * chunk, chunk)

    def send(src, dst, recv, device):
        sizes.append(math.prod(src.shape) * src.dtype.itemsize)
        copy(src, dst, sent.at[0], recv, device).start()

    def copy(src, dst, sem, recv, device):
        return pltpu.make_async_remote_copy(
            src_ref=src,
            dst_ref=dst,
            send_sem=sem,
            recv_sem=recv,
            device_id=device,
            device_id_type=MESH,
        )

    def arrived(like, recv):
        copy(like, like, recv, recv, x_dev).wait_recv()

    def landed(recv, *likes):
        total = sum(math.prod(like.shape) * like.dtype.itemsize for like in likes)
        arrived(gauge.at[pl.ds(0, total // (4 * width))], recv)

    barrier = pltpu.get_barrier_semaphore()
    across, mates = z_devs[: n_z // 2], z_devs[n_z // 2 :]
    peers = [x_dev, y_dev, p_dev] + mates
    for peer in peers:
        pl.semaphore_signal(barrier, inc=1, device_id=peer, device_id_type=MESH)

    @pl.when(high == 0)
    def _():
        for peer in across:
            pl.semaphore_signal(barrier, inc=1, device_id=peer, device_id_type=MESH)

    loads = [
        pltpu.make_async_copy(user_in, user_slot(col), load_sem.at[0]),
        pltpu.make_async_copy(item_in, i_got.at[:, 0], load_sem.at[1]),
        pltpu.make_async_copy(tile_in, tile_v, load_sem.at[2]),
        pltpu.make_async_copy(coords_in, coords, load_sem.at[3]),
            ]
    for load in loads:
        load.start()

    loads[3].wait()
    tu, ti = coords[0], coords[1]
    meta[0] = jnp.full(meta.shape[1:], tu, jnp.int32)
    meta[1] = jnp.full(meta.shape[1:], ti, jnp.int32)
    my_tu, my_ti = meta[0][0:1, :], meta[1][0:1, :]
    live = jnp.full((1, width), count_in[0, 0], jnp.int32) > 0
    pl.semaphore_wait(barrier, len(peers) + high * len(across))

    loads[0].wait()
    own = user_slot(col)

    @pl.when(high == 1)
    def _():
        for peer in across:
            pl.semaphore_signal(late, inc=1, device_id=peer, device_id_type=MESH)
        copy(own, own, first_s.at[0], uz_r.at[z], across[0]).start()

    sizes.extend([rows_u * width * 2] * (len(across) - 1))
    for device in mates:
        send(own, own, uz_r.at[z], device)
    for at, device in enumerate((x_dev, y_dev, p_dev)):
        send(meta, metas.at[at], io_r.at[0], device)
    loads[1].wait()
    for step in range(steps):
        for part, device in ((0, x_dev), (1, y_dev)):
            send(
                i_got.at[part, 0, rows_of(step)],
                r_near.at[part, rows_of(step)],
                iq_r.at[step],
                device,
            )
    send(own, own, up_r.at[0], p_dev)
    for part in range(2):
        send(i_got.at[part, 0], r_own.at[part], io_r.at[0], p_dev)

    loads[2].wait()
    tile_t[...] = tile_v[...].reshape(size, size).T
    @pl.when(high == 1)
    def _():
        copy(own, own, first_s.at[0], uz_r.at[z], across[0]).wait_send()
        for device in across[1:]:
            copy(own, own, sent.at[0], uz_r.at[z], device).start()

    landed(io_r.at[0], metas, r_own)
    x_ti, y_ti, p_ti = (metas[at, 1][0:1, :] for at in range(3))
    p_tu = metas[2, 0][0:1, :]

    def pass_user(at):
        slot = user_slot(2 * at + 1 - core)
        arrived(slot, uz_r.at[at])
        copy(slot, slot, sent.at[0], up_r.at[0], p_dev).start()

    def pass_items(step):
        landed(iq_r.at[step], r_near.at[:, rows_of(step)])
        for part, want, near, device in ((0, y_ti, row_x, y_dev), (1, x_ti, row_y, x_dev)):
            here = (part, rows_of(step))
            s_sel[here] = jnp.where(want == near, r_near[here], r_own[here])
            copy(
                s_sel.at[here], i_got.at[part, 2, rows_of(step)], sent.at[0], ig_r.at[0], device
            ).start()
            copy(
                r_near.at[here], i_got.at[part, 1, rows_of(step)], sent.at[0], ig_r.at[0], p_dev
            ).start()

    users = [(pass_user, at) for at in near_first]
    items = [(pass_items, step) for step in range(steps)]
    sizes.extend([rows_u * width * 2] * len(users) + [chunk * width * 2] * (4 * steps))

    for step, at in users[: len(mates)]:
        step(at)

    @pl.when(high == 0)
    def _():
        pl.semaphore_wait(late, len(across))
        for device in across[:0:-1]:
            copy(own, own, sent.at[0], uz_r.at[z], device).start()
        copy(own, own, first_s.at[0], uz_r.at[z], across[0]).start()

    for step, at in items:
        step(at)

    def pass_across():
        for step, at in users[len(mates) :]:
            step(at)


    def users_product():
        arrived(i_got.at[:, pl.ds(1, 2)], ig_r.at[0])
        sel_x = jnp.where(ti == row, 0, jnp.where(ti == row_x, 1, 2))
        sel_y = jnp.where(ti == row, 0, jnp.where(ti == row_y, 1, 2))
        item_sel = jnp.concatenate([i_got[0, sel_x], i_got[1, sel_y]], axis=0)
        item_sel = jnp.where(live, item_sel, 0.0).astype(item_sel.dtype)

        def multiply(some):
            rows = jnp.concatenate([tile_v[b] for b in some], axis=0)
            product = jnp.dot(rows, item_sel, preferred_element_type=jnp.float32)
            for at, b in enumerate(some):
                part_u[b] = product[at * rows_u : (at + 1) * rows_u]

        multiply([2 * h + core for h in turns])
        for h in turns:
            copy(part_u.at[2 * h + core], from_p.at[h], sent.at[0], rp_r.at[h], p_dev).start()
        multiply([2 * h + 1 - core for h in range(pieces)])

    def items_product():
        arrived(u_all.at[pl.ds(0, u_all.shape[0] // 2)], up_r.at[0])

        user_sel = u_all[tu]
        user_sel = jnp.where(live, user_sel, 0.0).astype(user_sel.dtype)
        for g in range(groups):
            rows = g * chunk * each
            lhs = [tile_t[part * half + rows : part * half + rows + chunk * each] for part in range(2)]
            product = jnp.dot(
                jnp.concatenate(lhs, axis=0), user_sel, preferred_element_type=jnp.float32
            )
            code, peak_1[g] = encode(product)
            some = slice(g * each, (g + 1) * each)
            send_1[:, some] = code.reshape(2, each, chunk, width)
            for part, device in enumerate((x_dev, y_dev)):
                copy(
                    peak_1.at[g], from_1p.at[part, g], sent.at[0], r1_r.at[g * each], device
                ).start()
            for step in range(g * each, (g + 1) * each):
                for part, device in enumerate((x_dev, y_dev)):
                    here = (part, step)
                    copy(
                        send_1.at[here], from_1.at[here], sent.at[0], r1_r.at[step], device
                    ).start()
            part_i[:, some] = product.reshape(2, each, chunk, width)
        copy(peak_1, pair_1p, sent.at[0], rq_r.at[0], p_dev).start()
        copy(send_1, pair_1, sent.at[0], rq_r.at[0], p_dev).start()

    for ref in (from_p, peak_1, peak_1, peak_1, send_1, send_1):
        sizes.append(math.prod(ref.shape) * ref.dtype.itemsize)

    targets = list(zip(others, z_devs))
    targets = targets[:1] + targets[n_z // 2 :] + [(z, p_dev)] + targets[1 : n_z // 2]

    def users_out(ready, some):
        for h in ready:
            arrived(from_p.at[h], rp_r.at[h])
        for at, device in some:
            tile, h = at // pieces, at % pieces
            send_z[at], peak_z[at] = encode(
                jnp.where(my_tu == tile, part_u[2 * h + 1 - core], 0.0)
                + jnp.where(p_tu == tile, from_p[h], 0.0)
            )
            copy(peak_z.at[at], from_zp.at[z], sent.at[0], rz_r.at[0], device).start()
            copy(send_z.at[at], from_z.at[z], sent.at[0], rz_r.at[0], device).start()

    def users_first():
        users_out(turns[:1], targets[:1])

    def users_rest():
        users_out(turns[1:], targets[1:])

    def items_out():
        landed(rq_r.at[0], pair_1, pair_1p)
        sides = ((0, x_ti, row_y, y_dev), (1, y_ti, row_x, x_dev))
        for step in range(steps):
            g = step // each
            if step % each == 0:
                landed(r1_r.at[step], from_1.at[:, step], from_1p.at[:, g])
                for part, other, owner, device in sides:
                    mask_1p[part, g] = jnp.where(other == row, from_1p[part, g], 0.0)
                    peak_2[part, g] = jnp.where(p_ti == owner, pair_1p[g], 0.0) + jnp.where(
                        other == owner, from_1p[part, g], TINY
                    )
                    copy(
                        peak_2.at[part, g], from_2p.at[part, g], sent.at[0], r2_r.at[step], device
                    ).start()
            else:
                landed(r1_r.at[step], from_1.at[:, step])
            for part, other, owner, device in sides:
                here = (part, step)
                send_2[here] = encode_by(
                    jnp.where(p_ti == owner, decode(pair_1[here], pair_1p[g]), 0.0)
                    + jnp.where(other == owner, decode(from_1[here], from_1p[part, g]), 0.0),
                    peak_2[part, g],
                )
                copy(
                    send_2.at[here], from_2.at[here], sent.at[0], r2_r.at[step], device
                ).start()
            for part in range(2):
                here = (part, step)
                copy(from_1.at[here], fwd_1.at[here], sent.at[0], r2_r.at[0], p_dev).start()
        copy(mask_1p, fwd_1p, sent.at[0], r2_r.at[0], p_dev).start()

    for ref in (peak_z, send_z, mask_1p, peak_2, send_2, from_1):
        sizes.append(math.prod(ref.shape) * ref.dtype.itemsize)

    def run(*stages):
        for stage in stages:
            stage()

    @pl.when(high == 0)
    def _():
        run(pass_across, items_product, users_product, users_first, users_rest, items_out)

    @pl.when(jnp.logical_and(high == 1, z < n_z - 1))
    def _():
        run(pass_across, users_product, items_product, users_first, users_rest, items_out)

    @pl.when(z == n_z - 1)
    def _():
        run(pass_across, users_product, users_first, items_product, users_rest, items_out)

    for step in range(steps):
        g = step // each
        if step == 0:
            landed(r2_r.at[0], from_2.at[:, 0], from_2p.at[:, 0], fwd_1, fwd_1p)
        elif step % each == 0:
            landed(r2_r.at[step], from_2.at[:, step], from_2p.at[:, g])
        else:
            landed(r2_r.at[step], from_2.at[:, step])
        for part in range(2):
            here = (part, step)
            last = jnp.where(my_ti == row, part_i[here], 0.0)
            last = last + decode(fwd_1[here], fwd_1p[part, g])
            last = last + decode(from_2[here], from_2p[part, g])
            start = part * half + step * chunk
            out_i[pl.ds(start, chunk), :] = last.astype(out_i.dtype)

    landed(rz_r.at[0], from_z, from_zp)
    total = decode(from_z[0], from_zp[0])
    for at in range(1, n_z):
        total = total + decode(from_z[at], from_zp[at])
    out_u[...] = total.astype(out_u.dtype)

    @pl.when(high == 0)
    def _():
        copy(own, own, first_s.at[0], uz_r.at[z], across[0]).wait_send()

    like = gauge.at[pl.ds(0, sum(sizes) // (4 * width))]
    copy(like, like, sent.at[0], sent.at[0], x_dev).wait_send()


def put(users, items, out_u, out_i, sems):
    copies = [
        pltpu.make_async_copy(users, out_u, sems.at[0]),
        pltpu.make_async_copy(items, out_i, sems.at[1]),
    ]
    for c in copies:
        c.start()
    for c in copies:
        c.wait()


def planned(user_feats, item_feats, tile_values, tile_coords, tile_count, *, n_z):
    rows_u, width = user_feats.shape
    rows_i = item_feats.shape[0]
    size = tile_values.shape[-1]
    f32, bf16, dma = jnp.float32, jnp.bfloat16, pltpu.SemaphoreType.DMA
    blocks = size // rows_u
    vmem = pl.BlockSpec(memory_space=pltpu.VMEM)
    anywhere = pl.BlockSpec(memory_space=pl.ANY)
    cut = (2, STEPS, rows_i // (2 * STEPS), width)
    peak = (1, width)
    tag = (8, width)
    i16 = jnp.int16
    vm = pltpu.VMEM
    outs = pl.pallas_call(
        functools.partial(kernel, n_z),
        out_shape=(pltpu.VMEM((rows_u, width), bf16), pltpu.VMEM((rows_i, width), bf16)),
        in_specs=[anywhere, pl.BlockSpec(memory_space=pltpu.SMEM)] + [anywhere] * 3,
        out_specs=(vmem, vmem),
        scratch_shapes=[
            vm((2 * n_z * rows_u // size, size, width), bf16),
            vm((2, 3, rows_i // 2, width), bf16),
            vm((2, rows_i // 2, width), bf16),
            vm((2, rows_i // 2, width), bf16),
            vm((2, rows_i // 2, width), bf16),
            vm((blocks, rows_u, size), bf16),
            vm((size, size), bf16),
            vm((2,) + tag, jnp.int32),
            vm((3, 2) + tag, jnp.int32),
            vm((blocks, rows_u, width), f32),
            vm((blocks // 2, rows_u, width), f32),
            vm((n_z, rows_u, width), i16),
            vm((n_z,) + peak, f32),
            vm((n_z, rows_u, width), i16),
            vm((n_z,) + peak, f32),
            vm(cut, f32),
            vm(cut, i16),
            vm((GROUPS,) + peak, f32),
            vm(cut, i16),
            vm((2, GROUPS) + peak, f32),
            vm(cut, i16),
            vm((GROUPS,) + peak, f32),
            vm(cut, i16),
            vm((2, GROUPS) + peak, f32),
            vm((2, GROUPS) + peak, f32),
            vm(cut, i16),
            vm((2, GROUPS) + peak, f32),
            vm(cut, i16),
            vm((2, GROUPS) + peak, f32),
            vm((16 * rows_i, width), f32),
            pltpu.SMEM((2,), jnp.int32),
        ]
        + [dma((n,)) for n in (4, 1, 1)]
        + [pltpu.SemaphoreType.REGULAR]
        + [dma((n,)) for n in (n_z, 1, 1, STEPS, 1, blocks // 2, 1, STEPS, 1, STEPS)],
        compiler_params=pltpu.CompilerParams(collective_id=0, has_side_effects=True),
    )(
        tile_coords.reshape(2),
        tile_count,
        user_feats,
        item_feats.reshape(2, rows_i // 2, width),
        tile_values.reshape(blocks, rows_u, size),
    )
    return pl.pallas_call(
        put,
        out_shape=[jax.ShapeDtypeStruct(out.shape, out.dtype) for out in outs],
        in_specs=[vmem, vmem],
        out_specs=[anywhere, anywhere],
        scratch_shapes=[dma((2,))],
    )(*[pltpu.with_memory_space_constraint(out, pltpu.VMEM) for out in outs])


def solution(mesh):
    n_row, n_col = mesh.shape["row"], mesh.shape["col"]

    def local(user_feats, item_feats, tile_values, tile_coords, tile_count):
        slots, size = tile_values.shape[2], tile_values.shape[3]
        rows_u = user_feats.shape[0]
        fits = (
            n_row == 4
            and n_col % 2 == 0
            and slots == 1
            and item_feats.shape[0] == size
            and size % (2 * rows_u) == 0
            and size % (32 * STEPS) == 0
            and n_col * rows_u % (2 * size) == 0
            and (n_col // 2 - 1) * rows_u <= size
        )
        args = (user_feats, item_feats, tile_values, tile_coords, tile_count)
        return planned(*args, n_z=n_col // 2) if fits else gathered(*args)

    placed = (
        P(("row", "col"), None),
        P(("col", "row"), None),
        P("row", "col", None, None, None),
        P("row", "col", None, None),
        P("row", "col"),
    )
    return jax.shard_map(
        local,
        mesh=mesh,
        in_specs=placed,
        out_specs=(P(("row", "col"), None), P(("col", "row"), None)),
        check_vma=False,
    )
```

```python
import functools
import math

import jax
import jax.numpy as jnp
from jax import lax
from jax.experimental import pallas as pl
from jax.experimental.pallas import tpu as pltpu
from jax.sharding import PartitionSpec as P

MESH = pl.DeviceIdType.MESH
LEVELS = 32760.0
STEPS = 8
GROUPS = 2
TINY = 1e-30


def gathered(user_feats, item_feats, tile_values, tile_coords, tile_count):
    user_block = lax.all_gather(user_feats, "col", axis=0, tiled=True)
    item_block = lax.all_gather(item_feats, "row", axis=0, tiled=True)
    tiles = tile_values[0, 0]
    coords = tile_coords[0, 0]
    count = tile_count[0, 0]
    slots = tiles.shape[0]
    size = tiles.shape[1]
    width = user_block.shape[1]
    user_tiles = user_block.shape[0] // size
    item_tiles = item_block.shape[0] // size
    live = jnp.arange(slots) < count
    pick_user = ((coords[0][:, None] == jnp.arange(user_tiles)[None, :]) & live[:, None]).astype(
        jnp.bfloat16
    )
    pick_item = (coords[1][:, None] == jnp.arange(item_tiles)[None, :]).astype(jnp.bfloat16)
    user_sel = jnp.einsum(
        "su,uiw->siw",
        pick_user,
        user_block.reshape(user_tiles, size, width),
        preferred_element_type=jnp.float32,
    ).astype(jnp.bfloat16)
    item_sel = jnp.einsum(
        "st,tjw->sjw",
        pick_item,
        item_block.reshape(item_tiles, size, width),
        preferred_element_type=jnp.float32,
    ).astype(jnp.bfloat16)
    to_users = jnp.einsum("sij,sjw->siw", tiles, item_sel, preferred_element_type=jnp.float32)
    to_items = jnp.einsum("sij,siw->sjw", tiles, user_sel, preferred_element_type=jnp.float32)
    part_users = jnp.einsum(
        "su,siw->uiw", pick_user.astype(jnp.float32), to_users, precision=lax.Precision.HIGHEST
    ).reshape(user_tiles * size, width)
    part_items = jnp.einsum(
        "st,sjw->tjw", pick_item.astype(jnp.float32), to_items, precision=lax.Precision.HIGHEST
    ).reshape(item_tiles * size, width)
    users_next = lax.psum_scatter(part_users, "col", scatter_dimension=0, tiled=True)
    items_next = lax.psum_scatter(part_items, "row", scatter_dimension=0, tiled=True)
    return (users_next.astype(jnp.bfloat16), items_next.astype(jnp.bfloat16))


def encode(values):
    rows, width = values.shape
    groups = values.reshape(rows // 8, 8, width)
    peak = jnp.max(jnp.max(jnp.abs(groups), axis=0), axis=0, keepdims=True)
    peak = jnp.maximum(peak, TINY)
    return encode_by(values, peak), peak


def encode_by(values, peak):
    rows, width = values.shape
    groups = values.reshape(rows // 8, 8, width)
    scaled = jnp.round(groups * (LEVELS / peak)[None])
    return scaled.astype(jnp.int32).astype(jnp.int16).reshape(rows, width)


def decode(code, peak):
    rows, width = code.shape
    groups = code.astype(jnp.int32).astype(jnp.float32).reshape(rows // 8, 8, width)
    return (groups * (peak * (1.0 / LEVELS))[None]).reshape(rows, width)


def kernel(
    n_z,
    coords_in,
    count_in,
    user_in,
    item_in,
    tile_in,
    out_u,
    out_i,
    u_all,
    i_got,
    r_own,
    r_near,
    s_sel,
    tile_v,
    tile_t,
    meta,
    metas,
    part_u,
    from_p,
    send_z,
    peak_z,
    from_z,
    from_zp,
    part_i,
    send_1,
    peak_1,
    from_1,
    from_1p,
    pair_1,
    pair_1p,
    fwd_1,
    mask_1p,
    fwd_1p,
    send_2,
    peak_2,
    from_2,
    from_2p,
    gauge,
    coords,
    load_sem,
    sent,
    first_s,
    late,
    uz_r,
    up_r,
    io_r,
    iq_r,
    ig_r,
    rp_r,
    rz_r,
    r1_r,
    rq_r,
    r2_r,
):
    row, col = lax.axis_index("row"), lax.axis_index("col")
    y, x = row // 2, row % 2
    z, core = col // 2, col % 2
    row_x, row_y = 2 * y + 1 - x, 2 * (1 - y) + x
    twin = 2 * z + 1 - core
    x_dev, y_dev, p_dev = (row_x, twin), (row_y, twin), (row, twin)
    high = z // (n_z // 2)

    def far_first(at):
        mirrored = z + high * (n_z - 1 - 2 * z)
        to = n_z - 1 - at
        to = jnp.where(to <= mirrored, to - 1, to)
        return to + high * (n_z - 1 - 2 * to)

    others = [far_first(at) for at in range(n_z - 1)]
    z_devs = [(row, 2 * at + 1 - core) for at in others]
    near_first = others[::-1]
    rows_u, rows_i = user_in.shape[0], i_got.shape[0] * i_got.shape[2]
    size = tile_v.shape[-1]
    width = user_in.shape[1]
    steps = send_1.shape[1]
    groups = peak_1.shape[0]
    half, each = rows_i // 2, steps // groups
    chunk = half // steps
    pieces = size // rows_u // 2
    turns = [(others[0] + step) % pieces for step in range(pieces)]
    sizes = []

    def user_slot(at):
        blocks = size // rows_u
        inner = pl.multiple_of(at % blocks * rows_u, rows_u)
        return u_all.at[at // blocks, pl.ds(inner, rows_u)]

    def rows_of(step):
        return pl.ds(step * chunk, chunk)

    def send(src, dst, recv, device):
        sizes.append(math.prod(src.shape) * src.dtype.itemsize)
        copy(src, dst, sent.at[0], recv, device).start()

    def copy(src, dst, sem, recv, device):
        return pltpu.make_async_remote_copy(
            src_ref=src,
            dst_ref=dst,
            send_sem=sem,
            recv_sem=recv,
            device_id=device,
            device_id_type=MESH,
        )

    def arrived(like, recv):
        copy(like, like, recv, recv, x_dev).wait_recv()

    def landed(recv, *likes):
        total = sum(math.prod(like.shape) * like.dtype.itemsize for like in likes)
        arrived(gauge.at[pl.ds(0, total // (4 * width))], recv)

    barrier = pltpu.get_barrier_semaphore()
    peers = [x_dev, y_dev, p_dev]
    for peer in peers:
        pl.semaphore_signal(barrier, inc=1, device_id=peer, device_id_type=MESH)
    for at, peer in zip(others, z_devs):

        @pl.when(at > z)
        def _():
            pl.semaphore_signal(barrier, inc=1, device_id=peer, device_id_type=MESH)

    loads = [
        pltpu.make_async_copy(user_in, user_slot(col), load_sem.at[0]),
        pltpu.make_async_copy(item_in, i_got.at[:, 0], load_sem.at[1]),
        pltpu.make_async_copy(tile_in, tile_v, load_sem.at[2]),
        pltpu.make_async_copy(coords_in, coords, load_sem.at[3]),
            ]
    for load in loads:
        load.start()

    loads[3].wait()
    tu, ti = coords[0], coords[1]
    meta[0] = jnp.full(meta.shape[1:], tu, jnp.int32)
    meta[1] = jnp.full(meta.shape[1:], ti, jnp.int32)
    my_tu, my_ti = meta[0][0:1, :], meta[1][0:1, :]
    live = jnp.full((1, width), count_in[0, 0], jnp.int32) > 0
    pl.semaphore_wait(barrier, len(peers) + z)

    loads[0].wait()
    own = user_slot(col)

    bottom, top = (row, 1 - core), (row, 2 * (n_z - 1) + 1 - core)

    def send_own(device, sem):
        copy(own, own, sem.at[0], uz_r.at[z], device).start()

    @pl.when(z > 0)
    def _():
        send_own(bottom, first_s)

    for at, peer in zip(others, z_devs):

        @pl.when(at < z)
        def _():
            pl.semaphore_signal(late, inc=1, device_id=peer, device_id_type=MESH)

    sizes.extend([rows_u * width * 2] * (n_z - 2))
    for at, device in enumerate((x_dev, y_dev, p_dev)):
        send(meta, metas.at[at], io_r.at[0], device)
    loads[1].wait()
    for step in range(steps):
        for part, device in ((0, x_dev), (1, y_dev)):
            send(
                i_got.at[part, 0, rows_of(step)],
                r_near.at[part, rows_of(step)],
                iq_r.at[step],
                device,
            )
    send(own, own, up_r.at[0], p_dev)
    for part in range(2):
        send(i_got.at[part, 0], r_own.at[part], io_r.at[0], p_dev)

    loads[2].wait()
    tile_t[...] = tile_v[...].reshape(size, size).T
    @pl.when(z > 0)
    def _():
        copy(own, own, first_s.at[0], uz_r.at[z], bottom).wait_send()

    for at, device in zip(others, z_devs):

        @pl.when(jnp.logical_and(at > 0, at < z))
        def _():
            send_own(device, sent)

    landed(io_r.at[0], metas, r_own)
    x_ti, y_ti, p_ti = (metas[at, 1][0:1, :] for at in range(3))
    p_tu = metas[2, 0][0:1, :]

    def pass_user(at):
        slot = user_slot(2 * at + 1 - core)
        arrived(slot, uz_r.at[at])
        copy(slot, slot, sent.at[0], up_r.at[0], p_dev).start()

    def pass_items(step):
        landed(iq_r.at[step], r_near.at[:, rows_of(step)])
        for part, want, near, device in ((0, y_ti, row_x, y_dev), (1, x_ti, row_y, x_dev)):
            here = (part, rows_of(step))
            s_sel[here] = jnp.where(want == near, r_near[here], r_own[here])
            copy(
                s_sel.at[here], i_got.at[part, 2, rows_of(step)], sent.at[0], ig_r.at[0], device
            ).start()
            copy(
                r_near.at[here], i_got.at[part, 1, rows_of(step)], sent.at[0], ig_r.at[0], p_dev
            ).start()

    users = [(pass_user, at) for at in near_first]
    items = [(pass_items, step) for step in range(steps)]
    sizes.extend([rows_u * width * 2] * len(users) + [chunk * width * 2] * (4 * steps))

    def send_up():
        @pl.when(z < n_z - 1)
        def _():
            pl.semaphore_wait(late, n_z - 1 - z)

        for at, device in list(zip(others, z_devs))[::-1]:

            @pl.when(jnp.logical_and(at > z, jnp.logical_or(z > 0, at < n_z - 1)))
            def _():
                send_own(device, sent)

        @pl.when(z == 0)
        def _():
            send_own(top, first_s)

    for step, at in items[: steps // 2]:
        step(at)
    send_up()
    for step, at in items[steps // 2 :]:
        step(at)

    def pass_across():
        for step, at in users:
            step(at)


    def users_product():
        arrived(i_got.at[:, pl.ds(1, 2)], ig_r.at[0])
        sel_x = jnp.where(ti == row, 0, jnp.where(ti == row_x, 1, 2))
        sel_y = jnp.where(ti == row, 0, jnp.where(ti == row_y, 1, 2))
        item_sel = jnp.concatenate([i_got[0, sel_x], i_got[1, sel_y]], axis=0)
        item_sel = jnp.where(live, item_sel, 0.0).astype(item_sel.dtype)

        def multiply(some):
            rows = jnp.concatenate([tile_v[b] for b in some], axis=0)
            product = jnp.dot(rows, item_sel, preferred_element_type=jnp.float32)
            for at, b in enumerate(some):
                part_u[b] = product[at * rows_u : (at + 1) * rows_u]

        multiply([2 * h + core for h in turns])
        for h in turns:
            copy(part_u.at[2 * h + core], from_p.at[h], sent.at[0], rp_r.at[h], p_dev).start()
        multiply([2 * h + 1 - core for h in range(pieces)])

    def items_product():
        arrived(u_all.at[pl.ds(0, u_all.shape[0] // 2)], up_r.at[0])

        user_sel = u_all[tu]
        user_sel = jnp.where(live, user_sel, 0.0).astype(user_sel.dtype)
        for g in range(groups):
            rows = g * chunk * each
            lhs = [tile_t[part * half + rows : part * half + rows + chunk * each] for part in range(2)]
            product = jnp.dot(
                jnp.concatenate(lhs, axis=0), user_sel, preferred_element_type=jnp.float32
            )
            code, peak_1[g] = encode(product)
            some = slice(g * each, (g + 1) * each)
            send_1[:, some] = code.reshape(2, each, chunk, width)
            for part, device in enumerate((x_dev, y_dev)):
                copy(
                    peak_1.at[g], from_1p.at[part, g], sent.at[0], r1_r.at[g * each], device
                ).start()
            for step in range(g * each, (g + 1) * each):
                for part, device in enumerate((x_dev, y_dev)):
                    here = (part, step)
                    copy(
                        send_1.at[here], from_1.at[here], sent.at[0], r1_r.at[step], device
                    ).start()
            part_i[:, some] = product.reshape(2, each, chunk, width)
        copy(peak_1, pair_1p, sent.at[0], rq_r.at[0], p_dev).start()
        copy(send_1, pair_1, sent.at[0], rq_r.at[0], p_dev).start()

    for ref in (from_p, peak_1, peak_1, peak_1, send_1, send_1):
        sizes.append(math.prod(ref.shape) * ref.dtype.itemsize)

    targets = list(zip(others, z_devs))
    targets = targets[:1] + targets[n_z // 2 :] + [(z, p_dev)] + targets[1 : n_z // 2]

    def users_out(ready, some):
        for h in ready:
            arrived(from_p.at[h], rp_r.at[h])
        for at, device in some:
            tile, h = at // pieces, at % pieces
            send_z[at], peak_z[at] = encode(
                jnp.where(my_tu == tile, part_u[2 * h + 1 - core], 0.0)
                + jnp.where(p_tu == tile, from_p[h], 0.0)
            )
            copy(peak_z.at[at], from_zp.at[z], sent.at[0], rz_r.at[0], device).start()
            copy(send_z.at[at], from_z.at[z], sent.at[0], rz_r.at[0], device).start()

    def users_first():
        users_out(turns[:1], targets[:1])

    def users_rest():
        users_out(turns[1:], targets[1:])

    def items_out():
        landed(rq_r.at[0], pair_1, pair_1p)
        sides = ((0, x_ti, row_y, y_dev), (1, y_ti, row_x, x_dev))
        for step in range(steps):
            g = step // each
            if step % each == 0:
                landed(r1_r.at[step], from_1.at[:, step], from_1p.at[:, g])
                for part, other, owner, device in sides:
                    mask_1p[part, g] = jnp.where(other == row, from_1p[part, g], 0.0)
                    peak_2[part, g] = jnp.where(p_ti == owner, pair_1p[g], 0.0) + jnp.where(
                        other == owner, from_1p[part, g], TINY
                    )
                    copy(
                        peak_2.at[part, g], from_2p.at[part, g], sent.at[0], r2_r.at[step], device
                    ).start()
            else:
                landed(r1_r.at[step], from_1.at[:, step])
            for part, other, owner, device in sides:
                here = (part, step)
                send_2[here] = encode_by(
                    jnp.where(p_ti == owner, decode(pair_1[here], pair_1p[g]), 0.0)
                    + jnp.where(other == owner, decode(from_1[here], from_1p[part, g]), 0.0),
                    peak_2[part, g],
                )
                copy(
                    send_2.at[here], from_2.at[here], sent.at[0], r2_r.at[step], device
                ).start()
            for part in range(2):
                here = (part, step)
                copy(from_1.at[here], fwd_1.at[here], sent.at[0], r2_r.at[0], p_dev).start()
        copy(mask_1p, fwd_1p, sent.at[0], r2_r.at[0], p_dev).start()

    for ref in (peak_z, send_z, mask_1p, peak_2, send_2, from_1):
        sizes.append(math.prod(ref.shape) * ref.dtype.itemsize)

    def run(*stages):
        for stage in stages:
            stage()

    @pl.when(high == 0)
    def _():
        run(pass_across, items_product, users_product, users_first, users_rest, items_out)

    @pl.when(jnp.logical_and(high == 1, z < n_z - 1))
    def _():
        run(pass_across, users_product, items_product, users_first, users_rest, items_out)

    @pl.when(z == n_z - 1)
    def _():
        run(users_product, pass_across, users_first, items_product, users_rest, items_out)

    for step in range(steps):
        g = step // each
        if step == 0:
            landed(r2_r.at[0], from_2.at[:, 0], from_2p.at[:, 0], fwd_1, fwd_1p)
        elif step % each == 0:
            landed(r2_r.at[step], from_2.at[:, step], from_2p.at[:, g])
        else:
            landed(r2_r.at[step], from_2.at[:, step])
        for part in range(2):
            here = (part, step)
            last = jnp.where(my_ti == row, part_i[here], 0.0)
            last = last + decode(fwd_1[here], fwd_1p[part, g])
            last = last + decode(from_2[here], from_2p[part, g])
            start = part * half + step * chunk
            out_i[pl.ds(start, chunk), :] = last.astype(out_i.dtype)

    landed(rz_r.at[0], from_z, from_zp)
    total = decode(from_z[0], from_zp[0])
    for at in range(1, n_z):
        total = total + decode(from_z[at], from_zp[at])
    out_u[...] = total.astype(out_u.dtype)

    @pl.when(z == 0)
    def _():
        copy(own, own, first_s.at[0], uz_r.at[z], top).wait_send()

    like = gauge.at[pl.ds(0, sum(sizes) // (4 * width))]
    copy(like, like, sent.at[0], sent.at[0], x_dev).wait_send()


def put(users, items, out_u, out_i, sems):
    copies = [
        pltpu.make_async_copy(users, out_u, sems.at[0]),
        pltpu.make_async_copy(items, out_i, sems.at[1]),
    ]
    for c in copies:
        c.start()
    for c in copies:
        c.wait()


def planned(user_feats, item_feats, tile_values, tile_coords, tile_count, *, n_z):
    rows_u, width = user_feats.shape
    rows_i = item_feats.shape[0]
    size = tile_values.shape[-1]
    f32, bf16, dma = jnp.float32, jnp.bfloat16, pltpu.SemaphoreType.DMA
    blocks = size // rows_u
    vmem = pl.BlockSpec(memory_space=pltpu.VMEM)
    anywhere = pl.BlockSpec(memory_space=pl.ANY)
    cut = (2, STEPS, rows_i // (2 * STEPS), width)
    peak = (1, width)
    tag = (8, width)
    i16 = jnp.int16
    vm = pltpu.VMEM
    outs = pl.pallas_call(
        functools.partial(kernel, n_z),
        out_shape=(pltpu.VMEM((rows_u, width), bf16), pltpu.VMEM((rows_i, width), bf16)),
        in_specs=[anywhere, pl.BlockSpec(memory_space=pltpu.SMEM)] + [anywhere] * 3,
        out_specs=(vmem, vmem),
        scratch_shapes=[
            vm((2 * n_z * rows_u // size, size, width), bf16),
            vm((2, 3, rows_i // 2, width), bf16),
            vm((2, rows_i // 2, width), bf16),
            vm((2, rows_i // 2, width), bf16),
            vm((2, rows_i // 2, width), bf16),
            vm((blocks, rows_u, size), bf16),
            vm((size, size), bf16),
            vm((2,) + tag, jnp.int32),
            vm((3, 2) + tag, jnp.int32),
            vm((blocks, rows_u, width), f32),
            vm((blocks // 2, rows_u, width), f32),
            vm((n_z, rows_u, width), i16),
            vm((n_z,) + peak, f32),
            vm((n_z, rows_u, width), i16),
            vm((n_z,) + peak, f32),
            vm(cut, f32),
            vm(cut, i16),
            vm((GROUPS,) + peak, f32),
            vm(cut, i16),
            vm((2, GROUPS) + peak, f32),
            vm(cut, i16),
            vm((GROUPS,) + peak, f32),
            vm(cut, i16),
            vm((2, GROUPS) + peak, f32),
            vm((2, GROUPS) + peak, f32),
            vm(cut, i16),
            vm((2, GROUPS) + peak, f32),
            vm(cut, i16),
            vm((2, GROUPS) + peak, f32),
            vm((16 * rows_i, width), f32),
            pltpu.SMEM((2,), jnp.int32),
        ]
        + [dma((n,)) for n in (4, 1, 1)]
        + [pltpu.SemaphoreType.REGULAR]
        + [dma((n,)) for n in (n_z, 1, 1, STEPS, 1, blocks // 2, 1, STEPS, 1, STEPS)],
        compiler_params=pltpu.CompilerParams(collective_id=0, has_side_effects=True),
    )(
        tile_coords.reshape(2),
        tile_count,
        user_feats,
        item_feats.reshape(2, rows_i // 2, width),
        tile_values.reshape(blocks, rows_u, size),
    )
    return pl.pallas_call(
        put,
        out_shape=[jax.ShapeDtypeStruct(out.shape, out.dtype) for out in outs],
        in_specs=[vmem, vmem],
        out_specs=[anywhere, anywhere],
        scratch_shapes=[dma((2,))],
    )(*[pltpu.with_memory_space_constraint(out, pltpu.VMEM) for out in outs])


def solution(mesh):
    n_row, n_col = mesh.shape["row"], mesh.shape["col"]

    def local(user_feats, item_feats, tile_values, tile_coords, tile_count):
        slots, size = tile_values.shape[2], tile_values.shape[3]
        rows_u = user_feats.shape[0]
        fits = (
            n_row == 4
            and n_col % 2 == 0
            and slots == 1
            and item_feats.shape[0] == size
            and size % (2 * rows_u) == 0
            and size % (32 * STEPS) == 0
            and n_col * rows_u % (2 * size) == 0
            and (n_col // 2 - 1) * rows_u <= size
        )
        args = (user_feats, item_feats, tile_values, tile_coords, tile_count)
        return planned(*args, n_z=n_col // 2) if fits else gathered(*args)

    placed = (
        P(("row", "col"), None),
        P(("col", "row"), None),
        P("row", "col", None, None, None),
        P("row", "col", None, None),
        P("row", "col"),
    )
    return jax.shard_map(
        local,
        mesh=mesh,
        in_specs=placed,
        out_specs=(P(("row", "col"), None), P(("col", "row"), None)),
        check_vma=False,
    )
```

```python
import functools
import math

import jax
import jax.numpy as jnp
from jax import lax
from jax.experimental import pallas as pl
from jax.experimental.pallas import tpu as pltpu
from jax.sharding import PartitionSpec as P

MESH = pl.DeviceIdType.MESH
LEVELS = 32760.0
STEPS = 8
GROUPS = 2
TINY = 1e-30


def gathered(user_feats, item_feats, tile_values, tile_coords, tile_count):
    user_block = lax.all_gather(user_feats, "col", axis=0, tiled=True)
    item_block = lax.all_gather(item_feats, "row", axis=0, tiled=True)
    tiles = tile_values[0, 0]
    coords = tile_coords[0, 0]
    count = tile_count[0, 0]
    slots = tiles.shape[0]
    size = tiles.shape[1]
    width = user_block.shape[1]
    user_tiles = user_block.shape[0] // size
    item_tiles = item_block.shape[0] // size
    live = jnp.arange(slots) < count
    pick_user = ((coords[0][:, None] == jnp.arange(user_tiles)[None, :]) & live[:, None]).astype(
        jnp.bfloat16
    )
    pick_item = (coords[1][:, None] == jnp.arange(item_tiles)[None, :]).astype(jnp.bfloat16)
    user_sel = jnp.einsum(
        "su,uiw->siw",
        pick_user,
        user_block.reshape(user_tiles, size, width),
        preferred_element_type=jnp.float32,
    ).astype(jnp.bfloat16)
    item_sel = jnp.einsum(
        "st,tjw->sjw",
        pick_item,
        item_block.reshape(item_tiles, size, width),
        preferred_element_type=jnp.float32,
    ).astype(jnp.bfloat16)
    to_users = jnp.einsum("sij,sjw->siw", tiles, item_sel, preferred_element_type=jnp.float32)
    to_items = jnp.einsum("sij,siw->sjw", tiles, user_sel, preferred_element_type=jnp.float32)
    part_users = jnp.einsum(
        "su,siw->uiw", pick_user.astype(jnp.float32), to_users, precision=lax.Precision.HIGHEST
    ).reshape(user_tiles * size, width)
    part_items = jnp.einsum(
        "st,sjw->tjw", pick_item.astype(jnp.float32), to_items, precision=lax.Precision.HIGHEST
    ).reshape(item_tiles * size, width)
    users_next = lax.psum_scatter(part_users, "col", scatter_dimension=0, tiled=True)
    items_next = lax.psum_scatter(part_items, "row", scatter_dimension=0, tiled=True)
    return (users_next.astype(jnp.bfloat16), items_next.astype(jnp.bfloat16))


def encode(values):
    rows, width = values.shape
    groups = values.reshape(rows // 8, 8, width)
    peak = jnp.max(jnp.max(jnp.abs(groups), axis=0), axis=0, keepdims=True)
    peak = jnp.maximum(peak, TINY)
    return encode_by(values, peak), peak


def encode_by(values, peak):
    rows, width = values.shape
    groups = values.reshape(rows // 8, 8, width)
    scaled = jnp.round(groups * (LEVELS / peak)[None])
    return scaled.astype(jnp.int32).astype(jnp.int16).reshape(rows, width)


def decode(code, peak):
    rows, width = code.shape
    groups = code.astype(jnp.int32).astype(jnp.float32).reshape(rows // 8, 8, width)
    return (groups * (peak * (1.0 / LEVELS))[None]).reshape(rows, width)


def kernel(
    n_z,
    coords_in,
    count_in,
    user_in,
    item_in,
    tile_in,
    out_u,
    out_i,
    u_all,
    i_got,
    r_own,
    r_near,
    s_sel,
    tile_v,
    tile_t,
    meta,
    metas,
    part_u,
    from_p,
    send_z,
    peak_z,
    from_z,
    from_zp,
    part_i,
    send_1,
    peak_1,
    from_1,
    from_1p,
    pair_1,
    pair_1p,
    fwd_1,
    mask_1p,
    fwd_1p,
    send_2,
    peak_2,
    from_2,
    from_2p,
    gauge,
    coords,
    load_sem,
    sent,
    first_s,
    late,
    uz_r,
    up_r,
    io_r,
    iq_r,
    ig_r,
    rp_r,
    rz_r,
    r1_r,
    rq_r,
    r2_r,
):
    row, col = lax.axis_index("row"), lax.axis_index("col")
    y, x = row // 2, row % 2
    z, core = col // 2, col % 2
    row_x, row_y = 2 * y + 1 - x, 2 * (1 - y) + x
    twin = 2 * z + 1 - core
    x_dev, y_dev, p_dev = (row_x, twin), (row_y, twin), (row, twin)
    high = z // (n_z // 2)

    def far_first(at):
        mirrored = z + high * (n_z - 1 - 2 * z)
        to = n_z - 1 - at
        to = jnp.where(to <= mirrored, to - 1, to)
        return to + high * (n_z - 1 - 2 * to)

    others = [far_first(at) for at in range(n_z - 1)]
    z_devs = [(row, 2 * at + 1 - core) for at in others]
    near_first = others[::-1]
    rows_u, rows_i = user_in.shape[0], i_got.shape[0] * i_got.shape[2]
    size = tile_v.shape[-1]
    width = user_in.shape[1]
    steps = send_1.shape[1]
    groups = peak_1.shape[0]
    half, each = rows_i // 2, steps // groups
    chunk = half // steps
    pieces = size // rows_u // 2
    turns = [(others[0] + step) % pieces for step in range(pieces)]
    sizes = []

    def user_slot(at):
        blocks = size // rows_u
        inner = pl.multiple_of(at % blocks * rows_u, rows_u)
        return u_all.at[at // blocks, pl.ds(inner, rows_u)]

    def rows_of(step):
        return pl.ds(step * chunk, chunk)

    def send(src, dst, recv, device):
        sizes.append(math.prod(src.shape) * src.dtype.itemsize)
        copy(src, dst, sent.at[0], recv, device).start()

    def copy(src, dst, sem, recv, device):
        return pltpu.make_async_remote_copy(
            src_ref=src,
            dst_ref=dst,
            send_sem=sem,
            recv_sem=recv,
            device_id=device,
            device_id_type=MESH,
        )

    def arrived(like, recv):
        copy(like, like, recv, recv, x_dev).wait_recv()

    def landed(recv, *likes):
        total = sum(math.prod(like.shape) * like.dtype.itemsize for like in likes)
        arrived(gauge.at[pl.ds(0, total // (4 * width))], recv)

    barrier = pltpu.get_barrier_semaphore()
    peers = [x_dev, y_dev, p_dev]
    for peer in peers:
        pl.semaphore_signal(barrier, inc=1, device_id=peer, device_id_type=MESH)
    for at, peer in zip(others, z_devs):

        @pl.when(at > z)
        def _():
            pl.semaphore_signal(barrier, inc=1, device_id=peer, device_id_type=MESH)

    loads = [
        pltpu.make_async_copy(user_in, user_slot(col), load_sem.at[0]),
        pltpu.make_async_copy(item_in, i_got.at[:, 0], load_sem.at[1]),
        pltpu.make_async_copy(tile_in, tile_v, load_sem.at[2]),
        pltpu.make_async_copy(coords_in, coords, load_sem.at[3]),
            ]
    for load in loads:
        load.start()

    loads[3].wait()
    tu, ti = coords[0], coords[1]
    meta[0] = jnp.full(meta.shape[1:], tu, jnp.int32)
    meta[1] = jnp.full(meta.shape[1:], ti, jnp.int32)
    my_tu, my_ti = meta[0][0:1, :], meta[1][0:1, :]
    live = jnp.full((1, width), count_in[0, 0], jnp.int32) > 0
    pl.semaphore_wait(barrier, len(peers) + z)

    loads[0].wait()
    own = user_slot(col)

    bottom, top = (row, 1 - core), (row, 2 * (n_z - 1) + 1 - core)

    def send_own(device, sem):
        copy(own, own, sem.at[0], uz_r.at[z], device).start()

    @pl.when(z > 0)
    def _():
        send_own(bottom, first_s)

    for at, peer in zip(others, z_devs):

        @pl.when(at < z)
        def _():
            pl.semaphore_signal(late, inc=1, device_id=peer, device_id_type=MESH)

    sizes.extend([rows_u * width * 2] * (n_z - 2))
    for at, device in enumerate((x_dev, y_dev, p_dev)):
        send(meta, metas.at[at], io_r.at[0], device)
    loads[1].wait()
    for step in range(steps):
        for part, device in ((0, x_dev), (1, y_dev)):
            send(
                i_got.at[part, 0, rows_of(step)],
                r_near.at[part, rows_of(step)],
                iq_r.at[step],
                device,
            )
    send(own, own, up_r.at[0], p_dev)
    for part in range(2):
        send(i_got.at[part, 0], r_own.at[part], io_r.at[0], p_dev)

    loads[2].wait()
    tile_t[...] = tile_v[...].reshape(size, size).T
    @pl.when(z > 0)
    def _():
        copy(own, own, first_s.at[0], uz_r.at[z], bottom).wait_send()

    for at, device in zip(others, z_devs):

        @pl.when(jnp.logical_and(at > 0, at < z))
        def _():
            send_own(device, sent)

    landed(io_r.at[0], metas, r_own)
    x_ti, y_ti, p_ti = (metas[at, 1][0:1, :] for at in range(3))
    p_tu = metas[2, 0][0:1, :]

    def pass_user(at):
        slot = user_slot(2 * at + 1 - core)
        arrived(slot, uz_r.at[at])
        copy(slot, slot, sent.at[0], up_r.at[0], p_dev).start()

    def pass_items(step):
        landed(iq_r.at[step], r_near.at[:, rows_of(step)])
        for part, want, near, device in ((0, y_ti, row_x, y_dev), (1, x_ti, row_y, x_dev)):
            here = (part, rows_of(step))
            s_sel[here] = jnp.where(want == near, r_near[here], r_own[here])
            copy(
                s_sel.at[here], i_got.at[part, 2, rows_of(step)], sent.at[0], ig_r.at[0], device
            ).start()
            copy(
                r_near.at[here], i_got.at[part, 1, rows_of(step)], sent.at[0], ig_r.at[0], p_dev
            ).start()

    users = [(pass_user, at) for at in near_first]
    items = [(pass_items, step) for step in range(steps)]
    sizes.extend([rows_u * width * 2] * len(users) + [chunk * width * 2] * (4 * steps))

    def send_up():
        @pl.when(z < n_z - 1)
        def _():
            pl.semaphore_wait(late, n_z - 1 - z)

        for at, device in list(zip(others, z_devs))[::-1]:

            @pl.when(jnp.logical_and(at > z, jnp.logical_or(z > 0, at < n_z - 1)))
            def _():
                send_own(device, sent)

        @pl.when(z == 0)
        def _():
            send_own(top, first_s)

    for step, at in items[: steps // 2]:
        step(at)
    send_up()
    for step, at in items[steps // 2 :]:
        step(at)

    def pass_across():
        for step, at in users:
            step(at)


    def users_product():
        arrived(i_got.at[:, pl.ds(1, 2)], ig_r.at[0])
        sel_x = jnp.where(ti == row, 0, jnp.where(ti == row_x, 1, 2))
        sel_y = jnp.where(ti == row, 0, jnp.where(ti == row_y, 1, 2))
        item_sel = jnp.concatenate([i_got[0, sel_x], i_got[1, sel_y]], axis=0)
        item_sel = jnp.where(live, item_sel, 0.0).astype(item_sel.dtype)

        def multiply(some):
            rows = jnp.concatenate([tile_v[b] for b in some], axis=0)
            product = jnp.dot(rows, item_sel, preferred_element_type=jnp.float32)
            for at, b in enumerate(some):
                part_u[b] = product[at * rows_u : (at + 1) * rows_u]

        multiply([2 * h + core for h in turns])
        for h in turns:
            copy(part_u.at[2 * h + core], from_p.at[h], sent.at[0], rp_r.at[h], p_dev).start()
        multiply([2 * h + 1 - core for h in range(pieces)])

    def items_product():
        arrived(u_all.at[pl.ds(0, u_all.shape[0] // 2)], up_r.at[0])

        user_sel = u_all[tu]
        user_sel = jnp.where(live, user_sel, 0.0).astype(user_sel.dtype)
        for g in range(groups):
            rows = g * chunk * each
            lhs = [tile_t[part * half + rows : part * half + rows + chunk * each] for part in range(2)]
            product = jnp.dot(
                jnp.concatenate(lhs, axis=0), user_sel, preferred_element_type=jnp.float32
            )
            code, peak_1[g] = encode(product)
            some = slice(g * each, (g + 1) * each)
            send_1[:, some] = code.reshape(2, each, chunk, width)
            for part, device in enumerate((x_dev, y_dev)):
                copy(
                    peak_1.at[g], from_1p.at[part, g], sent.at[0], r1_r.at[g * each], device
                ).start()
            for step in range(g * each, (g + 1) * each):
                for part, device in enumerate((x_dev, y_dev)):
                    here = (part, step)
                    copy(
                        send_1.at[here], from_1.at[here], sent.at[0], r1_r.at[step], device
                    ).start()
            part_i[:, some] = product.reshape(2, each, chunk, width)
        copy(peak_1, pair_1p, sent.at[0], rq_r.at[0], p_dev).start()
        copy(send_1, pair_1, sent.at[0], rq_r.at[0], p_dev).start()

    for ref in (from_p, peak_1, peak_1, peak_1, send_1, send_1):
        sizes.append(math.prod(ref.shape) * ref.dtype.itemsize)

    targets = list(zip(others, z_devs))
    targets = targets[:1] + targets[n_z // 2 :] + [(z, p_dev)] + targets[1 : n_z // 2]

    def users_out(ready, some):
        for h in ready:
            arrived(from_p.at[h], rp_r.at[h])
        for at, device in some:
            tile, h = at // pieces, at % pieces
            send_z[at], peak_z[at] = encode(
                jnp.where(my_tu == tile, part_u[2 * h + 1 - core], 0.0)
                + jnp.where(p_tu == tile, from_p[h], 0.0)
            )
            copy(peak_z.at[at], from_zp.at[z], sent.at[0], rz_r.at[0], device).start()
            copy(send_z.at[at], from_z.at[z], sent.at[0], rz_r.at[0], device).start()

    def users_first():
        users_out(turns[:1], targets[:1])

    def users_rest():
        users_out(turns[1:], targets[1:])

    def items_out():
        landed(rq_r.at[0], pair_1, pair_1p)
        sides = ((0, x_ti, row_y, y_dev), (1, y_ti, row_x, x_dev))
        for step in range(steps):
            g = step // each
            if step % each == 0:
                landed(r1_r.at[step], from_1.at[:, step], from_1p.at[:, g])
                for part, other, owner, device in sides:
                    mask_1p[part, g] = jnp.where(other == row, from_1p[part, g], 0.0)
                    peak_2[part, g] = jnp.where(p_ti == owner, pair_1p[g], 0.0) + jnp.where(
                        other == owner, from_1p[part, g], TINY
                    )
                    copy(
                        peak_2.at[part, g], from_2p.at[part, g], sent.at[0], r2_r.at[step], device
                    ).start()
            else:
                landed(r1_r.at[step], from_1.at[:, step])
            for part, other, owner, device in sides:
                here = (part, step)
                send_2[here] = encode_by(
                    jnp.where(p_ti == owner, decode(pair_1[here], pair_1p[g]), 0.0)
                    + jnp.where(other == owner, decode(from_1[here], from_1p[part, g]), 0.0),
                    peak_2[part, g],
                )
                copy(
                    send_2.at[here], from_2.at[here], sent.at[0], r2_r.at[step], device
                ).start()
            for part in range(2):
                here = (part, step)
                copy(from_1.at[here], fwd_1.at[here], sent.at[0], r2_r.at[0], p_dev).start()
        copy(mask_1p, fwd_1p, sent.at[0], r2_r.at[0], p_dev).start()

    for ref in (peak_z, send_z, mask_1p, peak_2, send_2, from_1):
        sizes.append(math.prod(ref.shape) * ref.dtype.itemsize)

    def run(*stages):
        for stage in stages:
            stage()

    @pl.when(high == 0)
    def _():
        run(pass_across, items_product, users_product, users_first, users_rest, items_out)

    @pl.when(jnp.logical_and(high == 1, z < n_z - 1))
    def _():
        run(users_product, pass_across, items_product, users_first, users_rest, items_out)

    @pl.when(z == n_z - 1)
    def _():
        run(users_product, pass_across, users_first, items_product, users_rest, items_out)

    for step in range(steps):
        g = step // each
        if step == 0:
            landed(r2_r.at[0], from_2.at[:, 0], from_2p.at[:, 0], fwd_1, fwd_1p)
        elif step % each == 0:
            landed(r2_r.at[step], from_2.at[:, step], from_2p.at[:, g])
        else:
            landed(r2_r.at[step], from_2.at[:, step])
        for part in range(2):
            here = (part, step)
            last = jnp.where(my_ti == row, part_i[here], 0.0)
            last = last + decode(fwd_1[here], fwd_1p[part, g])
            last = last + decode(from_2[here], from_2p[part, g])
            start = part * half + step * chunk
            out_i[pl.ds(start, chunk), :] = last.astype(out_i.dtype)

    landed(rz_r.at[0], from_z, from_zp)
    total = decode(from_z[0], from_zp[0])
    for at in range(1, n_z):
        total = total + decode(from_z[at], from_zp[at])
    out_u[...] = total.astype(out_u.dtype)

    @pl.when(z == 0)
    def _():
        copy(own, own, first_s.at[0], uz_r.at[z], top).wait_send()

    like = gauge.at[pl.ds(0, sum(sizes) // (4 * width))]
    copy(like, like, sent.at[0], sent.at[0], x_dev).wait_send()


def put(users, items, out_u, out_i, sems):
    copies = [
        pltpu.make_async_copy(users, out_u, sems.at[0]),
        pltpu.make_async_copy(items, out_i, sems.at[1]),
    ]
    for c in copies:
        c.start()
    for c in copies:
        c.wait()


def planned(user_feats, item_feats, tile_values, tile_coords, tile_count, *, n_z):
    rows_u, width = user_feats.shape
    rows_i = item_feats.shape[0]
    size = tile_values.shape[-1]
    f32, bf16, dma = jnp.float32, jnp.bfloat16, pltpu.SemaphoreType.DMA
    blocks = size // rows_u
    vmem = pl.BlockSpec(memory_space=pltpu.VMEM)
    anywhere = pl.BlockSpec(memory_space=pl.ANY)
    cut = (2, STEPS, rows_i // (2 * STEPS), width)
    peak = (1, width)
    tag = (8, width)
    i16 = jnp.int16
    vm = pltpu.VMEM
    outs = pl.pallas_call(
        functools.partial(kernel, n_z),
        out_shape=(pltpu.VMEM((rows_u, width), bf16), pltpu.VMEM((rows_i, width), bf16)),
        in_specs=[anywhere, pl.BlockSpec(memory_space=pltpu.SMEM)] + [anywhere] * 3,
        out_specs=(vmem, vmem),
        scratch_shapes=[
            vm((2 * n_z * rows_u // size, size, width), bf16),
            vm((2, 3, rows_i // 2, width), bf16),
            vm((2, rows_i // 2, width), bf16),
            vm((2, rows_i // 2, width), bf16),
            vm((2, rows_i // 2, width), bf16),
            vm((blocks, rows_u, size), bf16),
            vm((size, size), bf16),
            vm((2,) + tag, jnp.int32),
            vm((3, 2) + tag, jnp.int32),
            vm((blocks, rows_u, width), f32),
            vm((blocks // 2, rows_u, width), f32),
            vm((n_z, rows_u, width), i16),
            vm((n_z,) + peak, f32),
            vm((n_z, rows_u, width), i16),
            vm((n_z,) + peak, f32),
            vm(cut, f32),
            vm(cut, i16),
            vm((GROUPS,) + peak, f32),
            vm(cut, i16),
            vm((2, GROUPS) + peak, f32),
            vm(cut, i16),
            vm((GROUPS,) + peak, f32),
            vm(cut, i16),
            vm((2, GROUPS) + peak, f32),
            vm((2, GROUPS) + peak, f32),
            vm(cut, i16),
            vm((2, GROUPS) + peak, f32),
            vm(cut, i16),
            vm((2, GROUPS) + peak, f32),
            vm((16 * rows_i, width), f32),
            pltpu.SMEM((2,), jnp.int32),
        ]
        + [dma((n,)) for n in (4, 1, 1)]
        + [pltpu.SemaphoreType.REGULAR]
        + [dma((n,)) for n in (n_z, 1, 1, STEPS, 1, blocks // 2, 1, STEPS, 1, STEPS)],
        compiler_params=pltpu.CompilerParams(collective_id=0, has_side_effects=True),
    )(
        tile_coords.reshape(2),
        tile_count,
        user_feats,
        item_feats.reshape(2, rows_i // 2, width),
        tile_values.reshape(blocks, rows_u, size),
    )
    return pl.pallas_call(
        put,
        out_shape=[jax.ShapeDtypeStruct(out.shape, out.dtype) for out in outs],
        in_specs=[vmem, vmem],
        out_specs=[anywhere, anywhere],
        scratch_shapes=[dma((2,))],
    )(*[pltpu.with_memory_space_constraint(out, pltpu.VMEM) for out in outs])


def solution(mesh):
    n_row, n_col = mesh.shape["row"], mesh.shape["col"]

    def local(user_feats, item_feats, tile_values, tile_coords, tile_count):
        slots, size = tile_values.shape[2], tile_values.shape[3]
        rows_u = user_feats.shape[0]
        fits = (
            n_row == 4
            and n_col % 2 == 0
            and slots == 1
            and item_feats.shape[0] == size
            and size % (2 * rows_u) == 0
            and size % (32 * STEPS) == 0
            and n_col * rows_u % (2 * size) == 0
            and (n_col // 2 - 1) * rows_u <= size
        )
        args = (user_feats, item_feats, tile_values, tile_coords, tile_count)
        return planned(*args, n_z=n_col // 2) if fits else gathered(*args)

    placed = (
        P(("row", "col"), None),
        P(("col", "row"), None),
        P("row", "col", None, None, None),
        P("row", "col", None, None),
        P("row", "col"),
    )
    return jax.shard_map(
        local,
        mesh=mesh,
        in_specs=placed,
        out_specs=(P(("row", "col"), None), P(("col", "row"), None)),
        check_vma=False,
    )
```
